256 devices in a mesh: row: 16 (over z_lo, x, core), col: 16 (over y, z_hi).
Axes of the slice: x: 4, y: 4, z: 8 (z_hi: 4, z_lo: 2; z = z_hi * 2 + z_lo), core: 2. Of those that a mesh axis runs over, the one named last changes fastest.
Arguments:
- eigenvectors: float32 [8192, 2048], P('row', 'col'), may hold values from -6 to 6
- householder: float32 [3, 32, 512, 256], P(None, 'row', None, 'col'), may hold values from -6 to 6
Outputs:
- transformed: float32 [8192, 2048], P('row', 'col')
The draws below stay inside these ranges and needn't reach their ends.
All inputs are finite; a program needn't handle non-finite values.
Results may differ from the reference program's by a relative error of at most 0.0003.
Values sent between devices are 32-bit elements; how exact they have to be, the bound alone decides.
No kernel may reach another device: no remote copies, remote signals or barrier semaphores. Data moves between devices by JAX's collectives and lax.ppermute only.
A program may use at most 192 MiB of HBM per device.

```python
import jax
import jax.numpy as jnp
from jax import lax

REFL = 256
SWEEPS = 3
BLOCK_ROWS = 512
NBLOCKS = 32
NROWS = 8192
NCOLS = 2048


def steps_of(key, dims, shards, least, high):
    level, own = 1.0, jax.random.fold_in(key, 6)
    for dim, parts in shards:
        steps = jnp.exp(jax.random.uniform(jax.random.fold_in(own, dim), (parts,), jnp.float32, least / len(shards), high / len(shards)))
        level = level * jnp.repeat(steps, dims[dim] // parts).reshape([-1 if axis == dim else 1 for axis in range(len(dims))])
    return level


def scatter_about(stream_key, dims, deviation, bound, cuts=(), kind=jnp.bfloat16):
    result = jax.random.normal(stream_key, dims, jnp.float32) * deviation
    if len(cuts) > 0:
        result = steps_of(stream_key, dims, cuts, -0.22, 0.18) * result
    return jnp.clip(result, min=-bound, max=bound).astype(kind)


def setup_inputs(seed: int = 0) -> dict:
    keys = jax.random.split(jax.random.key(seed), 3)
    return {
        "eigenvectors": scatter_about(keys[0], (NROWS, NCOLS), 1.0, 6.0, ((0, 16), (1, 16)), jnp.float32),
        "householder": scatter_about(keys[1], (SWEEPS, NBLOCKS, BLOCK_ROWS, REFL), 1.0, 6.0, ((1, 16), (3, 16)), jnp.float32),
    }


PRECISE = lax.Precision.HIGHEST


def inner_product(left, right):
    return lax.dot_general(left, right, (((0,), (0,)), ((), ())), precision=PRECISE, preferred_element_type=jnp.float32)


def product(left, right):
    return jnp.dot(left, right, precision=PRECISE, preferred_element_type=jnp.float32)


def invert_upper(upper):
    order = upper.shape[0]
    rows_idx = lax.broadcasted_iota(jnp.int32, (order, order), 0)
    cols_idx = lax.broadcasted_iota(jnp.int32, (order, order), 1)
    inverse = jnp.where(rows_idx == cols_idx, 1.0 / jnp.diagonal(upper)[:, None], jnp.float32(0.0))
    size = 1
    while size < order:
        inside_old = (rows_idx // size) == (cols_idx // size)
        inside_new = (rows_idx // (2 * size)) == (cols_idx // (2 * size))
        corners = jnp.where(inside_new & jnp.logical_not(inside_old), upper, jnp.float32(0.0))
        inverse = inverse - product(product(inverse, corners), inverse)
        size = 2 * size
    return inverse


def reflect(stripe, vectors):
    gram_matrix = inner_product(vectors, vectors)
    upper_part = jnp.triu(gram_matrix, 1) + jnp.diag(jnp.diagonal(gram_matrix) * 0.5)
    weights = inner_product(vectors, stripe)
    scaled = product(invert_upper(upper_part), weights)
    return stripe - product(vectors, scaled)


def reference(eigenvectors, householder):
    matrix = eigenvectors
    for sweep_index in range(SWEEPS):
        sweep_vectors = householder[sweep_index]

        def apply_block(block_index, current):
            vectors = lax.dynamic_index_in_dim(sweep_vectors, block_index, 0, False)
            first_row = ((block_index - 1) * REFL).astype(jnp.int32)
            stripe = lax.dynamic_slice_in_dim(current, first_row, 2 * REFL, 0)
            return lax.dynamic_update_slice_in_dim(current, reflect(stripe, vectors), first_row, 0)

        matrix = lax.fori_loop(1, NBLOCKS, apply_block, matrix)
    return matrix
```

```python
import jax
import jax.numpy as jnp
from jax import lax
from jax.experimental import pallas as pl
from jax.experimental.pallas import tpu as pltpu
from jax.sharding import Mesh
from jax.sharding import PartitionSpec as P

ROW = ("zl", "x", "core")
CHIP = ("zl", "x")
COL = ("y", "zh")
SUBS = 2
INTERPRET = False

NN = (((1,), (0,)), ((), ()))
NT = (((1,), (1,)), ((), ()))
TN = (((0,), (0,)), ((), ()))


def split(value):
    high = value.astype(jnp.bfloat16)
    low = (value - high.astype(jnp.float32)).astype(jnp.bfloat16)
    return high, low


def dot3(left, right, dims=NN):
    def one(a, b):
        return lax.dot_general(a, b, dims, preferred_element_type=jnp.float32)

    return one(left[0], right[0]) + (one(left[0], right[1]) + one(left[1], right[0]))


def invert_upper(gram, valid):
    n = gram.shape[0]
    rows = lax.broadcasted_iota(jnp.int32, (n, n), 0)
    cols = lax.broadcasted_iota(jnp.int32, (n, n), 1)
    eye = rows == cols
    on_diagonal = jnp.where(eye, gram, 0.0)
    col_inverse = 1.0 / (0.5 * jnp.sum(on_diagonal, axis=1, keepdims=True))
    row_inverse = 1.0 / (0.5 * jnp.sum(on_diagonal, axis=0, keepdims=True))
    first = (rows // 2 == cols // 2) & (rows < cols)
    inverse = jnp.where(eye, col_inverse, 0.0)
    inverse = inverse - jnp.where(first, gram * col_inverse * row_inverse, 0.0)
    size = 2
    while 2 * size < n:
        corner = (rows // (2 * size) == cols // (2 * size)) & (rows // size < cols // size)
        edge = split(jnp.where(corner, gram, 0.0))
        parts = split(inverse)
        inverse = inverse - dot3(split(dot3(parts, edge)), parts)
        size = 2 * size
    upper = split(inverse[:size, :size])
    lower = split(inverse[size:, size:])
    corner = dot3(split(dot3(upper, split(gram[:size, size:]))), lower)
    return inverse, corner


def prepare_body(index_ref, near_ref, after_ref, before_ref, far0_ref, far1_ref, high_ref, low_ref, v_ref):
    blocks, quarter, m = near_ref.shape
    n = 4 * quarter
    piece = quarter // 4
    at_y = index_ref[0]
    at_z = index_ref[1]
    for block in range(blocks):
        far = far0_ref if block == 0 else far1_ref
        for dy in range(4):
            base = lax.rem(at_y + dy, 4) * quarter
            for dz in range(4):
                start = base + lax.rem(at_z + dz, 4) * piece
                rows = pl.ds(dz * piece, piece)
                if dy == 0:
                    part = near_ref[block, rows, :]
                elif dy == 1:
                    part = after_ref[block, rows, :]
                elif dy == 2:
                    part = far[rows, :]
                else:
                    part = before_ref[block, rows, :]
                v_ref[block, pl.ds(start, piece), :] = part
    eye = lax.broadcasted_iota(jnp.int32, (m, m), 0) == lax.broadcasted_iota(jnp.int32, (m, m), 1)
    unit = jnp.where(eye, 1.0, 0.0)
    half = n // 2
    for block in range(blocks):
        valid = index_ref[2 + block] == 1
        vectors = split(v_ref[block])
        gram = dot3(vectors, vectors, NT)
        inverse, corner = invert_upper(gram, valid)
        up = split(inverse[:half, :half])
        down = split(inverse[half:, half:])
        edge = split(corner)
        v_up = (vectors[0][:half], vectors[1][:half])
        v_down = (vectors[0][half:], vectors[1][half:])
        lower = dot3(down, v_down)
        upper = dot3(up, v_up) - dot3(edge, v_down)
        scaled = split(jnp.concatenate([upper, lower], axis=0))
        whole = unit - dot3(scaled, vectors, TN)
        whole = jnp.where(valid, whole, unit)
        high, low = split(whole)
        high_ref[block] = high
        low_ref[block] = low


def prepare(index, near, after, before, far0, far1):
    blocks, quarter, m = near.shape
    out = jax.ShapeDtypeStruct((blocks, m, m), jnp.bfloat16)
    vmem = pl.BlockSpec(memory_space=pltpu.VMEM)
    return pl.pallas_call(
        prepare_body,
        out_shape=(out, out),
        in_specs=[pl.BlockSpec(memory_space=pltpu.SMEM)] + [vmem] * 5,
        out_specs=(vmem, vmem),
        scratch_shapes=[pltpu.VMEM((blocks, 4 * quarter, m), jnp.float32)],
        compiler_params=pltpu.CompilerParams(vmem_limit_bytes=40 * 1024 * 1024),
        interpret=INTERPRET,
        name="prepare",
    )(index, near, after, before, far0, far1)


def operate_body(first_ref, data_ref, own_ref, h0, l0, h1, l1, h2, l2, map_ref, add_ref):
    n = h0.shape[1] // 2
    first = first_ref[0] == 1
    width = data_ref.shape[0]
    sweeps = ((h0, l0), (h1, l1), (h2, l2))

    def part(sweep, block, rows=None):
        high, low = sweeps[sweep]
        if rows is None:
            return high[block], low[block]
        at = pl.ds(rows * n, n)
        return high[block, at, :], low[block, at, :]

    extra = dot3(split(own_ref[...]), part(2, 0))
    own = data_ref[...]
    start = jnp.where(first, extra, 0.0)
    incoming = (start[:, n:], start[:, :n], jnp.zeros((width, n), jnp.float32))
    zeros = jnp.zeros((n, n), jnp.float32)
    for sweep in range(3):
        a = part(sweep, 0)
        if sweep == 2:
            size = 2 * n
            eye = lax.broadcasted_iota(jnp.int32, (size, size), 0) == lax.broadcasted_iota(jnp.int32, (size, size), 1)
            a = (
                jnp.where(first, eye.astype(jnp.float32), a[0].astype(jnp.float32)).astype(jnp.bfloat16),
                jnp.where(first, 0.0, a[1].astype(jnp.float32)).astype(jnp.bfloat16),
            )
        a_top = (a[0][:n], a[1][:n])
        a_low = (a[0][n:], a[1][n:])
        b_top = part(sweep, 1, 0)
        b_low = part(sweep, 1, 1)
        fresh = a_top[0].astype(jnp.float32) + a_top[1].astype(jnp.float32)
        if sweep == 0:
            u, v = own[:, :n], own[:, n:]
            mid = dot3(split(incoming[0]), a_top) + dot3(split(u), a_low)
            mid = jnp.concatenate([fresh, mid], axis=0)
            done = dot3(split(mid[:, n:]), b_top)
            last = dot3(split(v), b_low)
            done = jnp.concatenate([done[:n], done[n:] + last], axis=0)
        else:
            mid = dot3(split(u), a_low)
            data = mid[-width:] + dot3(split(incoming[sweep]), a_top)
            mid = jnp.concatenate([mid[:-width], data, fresh], axis=0)
            done = dot3(split(mid[:, n:]), b_top)
            last = dot3(split(v), b_low)
            count = last.shape[0]
            done = jnp.concatenate([done[:count] + last, done[count:]], axis=0)
            def reorder(value):
                return jnp.concatenate([value[: count - width], value[count:], value[count - width : count]], axis=0)
            mid = reorder(mid)
            done = reorder(done)
        known = (sweep + 1) * n
        u, v = mid[:, :n], done[:, :n]
        out = done[:, n:]
        map_ref[0:known, sweep * n : (sweep + 1) * n] = out[:known]
        for later in range(sweep + 1, 3):
            map_ref[later * n : (later + 1) * n, sweep * n : (sweep + 1) * n] = zeros
        add_ref[:, sweep * n : (sweep + 1) * n] = out[known:]
    map_ref[:, 3 * n : 4 * n] = u[: 3 * n]
    map_ref[:, 4 * n : 5 * n] = v[: 3 * n]
    add_ref[:, 3 * n : 4 * n] = u[3 * n :]
    add_ref[:, 4 * n : 5 * n] = v[3 * n :]


def operate(first, data, own, parts):
    width, m = data.shape
    n = m // 2
    vmem = pl.BlockSpec(memory_space=pltpu.VMEM)
    return pl.pallas_call(
        operate_body,
        out_shape=(
            jax.ShapeDtypeStruct((3 * n, 5 * n), jnp.float32),
            jax.ShapeDtypeStruct((width, 5 * n), jnp.float32),
        ),
        in_specs=[pl.BlockSpec(memory_space=pltpu.SMEM)] + [vmem] * 8,
        out_specs=(vmem, vmem),
        compiler_params=pltpu.CompilerParams(vmem_limit_bytes=48 * 1024 * 1024),
        interpret=INTERPRET,
        name="operate",
    )(first, data, own, *parts)


def product(left, right):
    return jnp.dot(left, right, precision=lax.Precision.HIGH, preferred_element_type=jnp.float32)


def ring(value, axis, step):
    count = lax.axis_size(axis)
    return lax.ppermute(value, axis, [(k, (k + step) % count) for k in range(count)])


def from_next(value):
    count = lax.axis_size(ROW)
    return lax.ppermute(value, ROW, [(k + 1, k) for k in range(count - 1)])


def gather_pieces(value):
    before = ring(value, "zh", 1)
    after = ring(value, "zh", -1)
    far0 = ring(before[0], "zh", 1)
    far1 = ring(after[1], "zh", -1)
    near = jnp.concatenate([value, after, jnp.stack([far0, far1]), before], axis=1)
    before = ring(near, "y", 1)
    after = ring(near, "y", -1)
    far0 = ring(before[0], "y", 1)
    far1 = ring(after[1], "y", -1)
    return near, after, before, far0, far1


def shards(eigenvectors, householder):
    position = lax.axis_index(ROW)
    count = lax.axis_size(ROW)
    is_first = position == 0
    is_last = position == count - 1
    is_odd = lax.axis_index("core") == 1
    n = eigenvectors.shape[0] // 2
    local = jnp.swapaxes(householder, 2, 3)
    moved = from_next(jnp.concatenate([local[0], local[1, :1]], axis=0))
    data = from_next(eigenvectors)
    own2 = jnp.where(is_first, jnp.stack([local[0, 1], local[2, 1]]), local[2])
    own1 = jnp.stack([local[1, 1], moved[2]])
    own0 = moved[:2]
    at = [lax.axis_index("y"), lax.axis_index("zh")]
    one = jnp.int32(1)
    present = jnp.where(is_last, 0, 1).astype(jnp.int32)

    def index(*valid):
        return jnp.stack([*at, *valid]).astype(jnp.int32)

    parts2 = prepare(index(one, one), *gather_pieces(own2))
    parts1 = prepare(index(one, present), *gather_pieces(own1))
    parts0 = prepare(index(present, present), *gather_pieces(own0))
    first = is_first.astype(jnp.int32).reshape(1)
    mapping, add = operate(first, data.T, eigenvectors.T, (*parts0, *parts1, *parts2))

    swap = [(0, 1), (1, 0)]
    step = mapping[:, : 3 * n]
    width = add.shape[0]
    half = width // 2
    other_step = lax.ppermute(step, "core", swap)
    halves = add[:, : 3 * n].reshape(2, half, 3 * n)
    keep = jnp.where(is_odd, halves[1], halves[0])
    give = jnp.where(is_odd, halves[0], halves[1])
    got = lax.ppermute(give, "core", swap)
    even_step = jnp.where(is_odd, other_step, step)
    odd_step = jnp.where(is_odd, step, other_step)
    even_add = jnp.where(is_odd, got, keep)
    odd_add = jnp.where(is_odd, keep, got)
    chip_step = product(even_step, odd_step)
    chip_add = product(even_add, odd_step) + odd_add

    chips = lax.axis_size(CHIP)
    sub = half // SUBS
    adds = [chip_add[k * sub : (k + 1) * sub] for k in range(SUBS)]
    states = [None] * SUBS
    for hop in range(1, chips):
        for k in range(SUBS):
            sent = adds[k] if hop == 1 else product(states[k], chip_step) + adds[k]
            arrived = lax.ppermute(sent, CHIP, [(hop - 1, hop)])
            states[k] = arrived if hop == 1 else states[k] + arrived
    state = jnp.concatenate(states, axis=0)
    odd_state = product(state, even_step) + even_add
    got = lax.ppermute(jnp.where(is_odd, state, odd_state), "core", swap)
    state = jnp.where(
        is_odd, jnp.concatenate([got, odd_state], axis=0), jnp.concatenate([state, got], axis=0)
    )
    final = product(state, mapping[:, 2 * n :]) + add[:, 2 * n :]
    handed = from_next(final[:, n : 2 * n])
    lower = jnp.where(is_last, final[:, :n], handed)
    return jnp.concatenate([final[:, 2 * n :], lower], axis=1).T


def solution(mesh):
    split_mesh = Mesh(mesh.devices.reshape(2, 4, 2, 4, 4), (*ROW, *COL))
    return jax.shard_map(
        shards,
        mesh=split_mesh,
        in_specs=(P(ROW, COL), P(None, ROW, None, COL)),
        out_specs=P(ROW, COL),
        check_vma=False,
    )
```

```python
import jax
import jax.numpy as jnp
from jax import lax
from jax.experimental import pallas as pl
from jax.experimental.pallas import tpu as pltpu
from jax.sharding import Mesh
from jax.sharding import PartitionSpec as P

ROW = ("zl", "x", "core")
CHIP = ("zl", "x")
COL = ("y", "zh")
SUBS = 2
INTERPRET = False

NN = (((1,), (0,)), ((), ()))
NT = (((1,), (1,)), ((), ()))
TN = (((0,), (0,)), ((), ()))


def split(value):
    high = value.astype(jnp.bfloat16)
    low = (value - high.astype(jnp.float32)).astype(jnp.bfloat16)
    return high, low


def dot3(left, right, dims=NN):
    (on_left,), (on_right,) = dims[0]
    long_left = jnp.concatenate([left[0], left[0], left[1]], axis=on_left)
    long_right = jnp.concatenate([right[0], right[1], right[0]], axis=on_right)
    return lax.dot_general(long_left, long_right, dims, preferred_element_type=jnp.float32)


def prepare_body(index_ref, near_ref, after_ref, before_ref, far0_ref, far1_ref, high_ref, low_ref, v_ref, g_ref, p_ref):
    blocks, quarter, m = near_ref.shape
    n = 4 * quarter
    half = n // 2
    piece = quarter // 4
    at_y = index_ref[0]
    at_z = index_ref[1]
    valid = index_ref[2] == 1
    for block in range(blocks):
        for dy in range(4):
            base = lax.rem(at_y + dy, 4) * quarter
            for dz in range(4):
                start = base + lax.rem(at_z + dz, 4) * piece
                at = pl.ds(dz * piece, piece)
                if dy == 0:
                    part = near_ref[block, at, :]
                elif dy == 1:
                    part = after_ref[block, at, :]
                elif dy == 3:
                    part = before_ref[block, at, :]
                elif dz < 2:
                    part = far0_ref[block, at, :]
                else:
                    part = far1_ref[block, pl.ds((dz - 2) * piece, piece), :]
                v_ref[block, pl.ds(start, piece), :] = part
    rows = lax.broadcasted_iota(jnp.int32, (half, half), 0)
    cols = lax.broadcasted_iota(jnp.int32, (half, half), 1)
    eye = rows == cols
    pair = (rows // 2 == cols // 2) & (rows < cols)
    for block in range(blocks):
        vectors = split(v_ref[block])
        g_ref[block] = dot3(vectors, vectors, NT)
    problems = [(block, side) for block in range(blocks) for side in range(2)]
    for at, (block, side) in enumerate(problems):
        lo = side * half
        gram = g_ref[block, lo : lo + half, lo : lo + half]
        on_diagonal = jnp.where(eye, gram, 0.0)
        col_inverse = 1.0 / (0.5 * jnp.sum(on_diagonal, axis=1, keepdims=True))
        row_inverse = 1.0 / (0.5 * jnp.sum(on_diagonal, axis=0, keepdims=True))
        inverse = jnp.where(eye, col_inverse, 0.0)
        p_ref[at] = inverse - jnp.where(pair, gram * col_inverse * row_inverse, 0.0)

    levels = half.bit_length() - 1

    def level(power, carry):
        old_rows = jnp.right_shift(rows, power)
        old_cols = jnp.right_shift(cols, power)
        corner = (jnp.right_shift(old_rows, 1) == jnp.right_shift(old_cols, 1)) & (old_rows < old_cols)
        first = []
        for at, (block, side) in enumerate(problems):
            lo = side * half
            edge = split(jnp.where(corner, g_ref[block, lo : lo + half, lo : lo + half], 0.0))
            first.append(dot3(split(p_ref[at]), edge))
        for at in range(len(problems)):
            old = p_ref[at]
            p_ref[at] = old - dot3(split(first[at]), split(old))
        return carry

    lax.fori_loop(1, levels, level, 0)
    eye = lax.broadcasted_iota(jnp.int32, (m, m), 0) == lax.broadcasted_iota(jnp.int32, (m, m), 1)
    unit = jnp.where(eye, 1.0, 0.0)
    first = [
        dot3(split(p_ref[2 * block]), split(g_ref[block, :half, half:])) for block in range(blocks)
    ]
    corners = [dot3(split(first[block]), split(p_ref[2 * block + 1])) for block in range(blocks)]
    for block in range(blocks):
        vectors = split(v_ref[block])
        top = split(jnp.concatenate([p_ref[2 * block], -corners[block]], axis=1))
        low = split(p_ref[2 * block + 1])
        upper = dot3(top, vectors)
        lower = dot3(low, (vectors[0][half:], vectors[1][half:]))
        scaled = split(jnp.concatenate([upper, lower], axis=0).T)
        whole = unit - dot3(scaled, vectors)
        whole = jnp.where(valid, whole, unit)
        high, low = split(whole)
        high_ref[block] = high
        low_ref[block] = low


def prepare(index, near, after, before, far0, far1):
    blocks, quarter, m = near.shape
    n = 4 * quarter
    out = jax.ShapeDtypeStruct((blocks, m, m), jnp.bfloat16)
    vmem = pl.BlockSpec(memory_space=pltpu.VMEM)
    return pl.pallas_call(
        prepare_body,
        out_shape=(out, out),
        in_specs=[pl.BlockSpec(memory_space=pltpu.SMEM)] + [vmem] * 5,
        out_specs=(vmem, vmem),
        scratch_shapes=[
            pltpu.VMEM((blocks, n, m), jnp.float32),
            pltpu.VMEM((blocks, n, n), jnp.float32),
            pltpu.VMEM((2 * blocks, n // 2, n // 2), jnp.float32),
        ],
        compiler_params=pltpu.CompilerParams(vmem_limit_bytes=40 * 1024 * 1024),
        cost_estimate=pl.CostEstimate(flops=2_000_000_000, bytes_accessed=1_000_000, transcendentals=0),
        interpret=INTERPRET,
        name="prepare",
    )(index, near, after, before, far0, far1)


PAIRS = ((0, 0), (0, 1), (0, 2), (1, 1), (1, 2), (2, 2))


def operate_body(first_ref, data_ref, own_ref, ah, al, bh, bl, step_ref, rest_ref, add_ref):
    n = ah.shape[1] // 2
    first = first_ref[0] == 1
    width = data_ref.shape[0]
    where_held = {(0, 0): (bh, bl, 0), (0, 1): (bh, bl, 1), (1, 0): (ah, al, 2), (1, 1): (bh, bl, 2), (2, 0): (ah, al, 0), (2, 1): (ah, al, 1)}

    def part(sweep, block, side=None):
        high, low, at = where_held[sweep, block]
        if side is None:
            return high[at], low[at]
        rows = pl.ds(side * n, n)
        return high[at, rows, :], low[at, rows, :]

    extra = dot3(split(own_ref[...]), part(2, 0))
    own = data_ref[...]
    start = jnp.where(first, extra, 0.0)
    incoming = (start[:, n:], start[:, :n], jnp.zeros((width, n), jnp.float32))
    for sweep in range(3):
        a = part(sweep, 0)
        if sweep == 2:
            size = 2 * n
            eye = lax.broadcasted_iota(jnp.int32, (size, size), 0) == lax.broadcasted_iota(jnp.int32, (size, size), 1)
            a = (
                jnp.where(first, eye.astype(jnp.float32), a[0].astype(jnp.float32)).astype(jnp.bfloat16),
                jnp.where(first, 0.0, a[1].astype(jnp.float32)).astype(jnp.bfloat16),
            )
        a_top = (a[0][:n], a[1][:n])
        a_low = (a[0][n:], a[1][n:])
        b_top = part(sweep, 1, 0)
        b_low = part(sweep, 1, 1)
        fresh = a_top[0].astype(jnp.float32) + a_top[1].astype(jnp.float32)
        if sweep == 0:
            u, v = own[:, :n], own[:, n:]
            mid = dot3(split(jnp.concatenate([incoming[0], u], axis=1)), a)
            mid = jnp.concatenate([fresh, mid], axis=0)
            done = dot3(split(mid[:, n:]), b_top)
            last = dot3(split(v), b_low)
            done = jnp.concatenate([done[:n], done[n:] + last], axis=0)
        else:
            mid = dot3(split(u), a_low)
            if sweep == 1:
                data = mid[-width:] + dot3(split(incoming[sweep]), a_top)
                mid = jnp.concatenate([mid[:-width], fresh, data], axis=0)
            else:
                mid = jnp.concatenate([mid[:-width], fresh, mid[-width:]], axis=0)
            done = dot3(split(mid[:, n:]), b_top)
            last = dot3(split(v), b_low)
            early = sweep * n
            done = jnp.concatenate(
                [done[:early] + last[:early], done[early : early + n], done[early + n :] + last[early:]], axis=0
            )
        known = (sweep + 1) * n
        u, v = mid[:, :n], done[:, :n]
        out = done[:, n:]
        for k in range(sweep + 1):
            step_ref[PAIRS.index((k, sweep))] = out[k * n : (k + 1) * n]
        add_ref[:, sweep * n : (sweep + 1) * n] = out[known:]
    rest_ref[:, 0:n] = out[: 3 * n]
    rest_ref[:, n : 2 * n] = u[: 3 * n]
    rest_ref[:, 2 * n : 3 * n] = v[: 3 * n]
    add_ref[:, 3 * n : 4 * n] = u[3 * n :]
    add_ref[:, 4 * n : 5 * n] = v[3 * n :]


def operate(first, data, own, parts):
    width, m = data.shape
    n = m // 2
    vmem = pl.BlockSpec(memory_space=pltpu.VMEM)
    return pl.pallas_call(
        operate_body,
        out_shape=(
            jax.ShapeDtypeStruct((6, n, n), jnp.float32),
            jax.ShapeDtypeStruct((3 * n, 3 * n), jnp.float32),
            jax.ShapeDtypeStruct((width, 5 * n), jnp.float32),
        ),
        in_specs=[pl.BlockSpec(memory_space=pltpu.SMEM)] + [vmem] * 6,
        out_specs=(vmem,) * 3,
        compiler_params=pltpu.CompilerParams(vmem_limit_bytes=48 * 1024 * 1024),
        interpret=INTERPRET,
        name="operate",
    )(first, data, own, *parts)


def merge_body(odd_ref, mine_ref, other_ref, keep_ref, got_ref, high_ref, low_ref, add_ref, even_ref, even_add_ref):
    n = mine_ref.shape[1]
    odd = odd_ref[0] == 1
    mine = mine_ref[...]
    other = other_ref[...]
    evens = jnp.where(odd, other, mine)
    odds = jnp.where(odd, mine, other)
    keep = keep_ref[...]
    got = got_ref[...]
    even_add = jnp.where(odd, got, keep)
    odd_add = jnp.where(odd, keep, got)
    even_add_ref[...] = even_add
    even_parts = [split(evens[k]) for k in range(6)]
    odd_parts = [split(odds[k]) for k in range(6)]
    add_parts = split(even_add)
    even_ref[...] = jnp.zeros(even_ref.shape, jnp.float32)
    for s in range(3):
        total = odd_add[:, s * n : (s + 1) * n]
        for j in range(s + 1):
            columns = slice(j * n, (j + 1) * n)
            total = total + dot3((add_parts[0][:, columns], add_parts[1][:, columns]), odd_parts[PAIRS.index((j, s))])
        add_ref[:, s * n : (s + 1) * n] = total
        for k in range(s + 1):
            even_ref[k * n : (k + 1) * n, s * n : (s + 1) * n] = evens[PAIRS.index((k, s))]
            total = None
            for j in range(k, s + 1):
                term = dot3(even_parts[PAIRS.index((k, j))], odd_parts[PAIRS.index((j, s))])
                total = term if total is None else total + term
            high_ref[PAIRS.index((k, s))], low_ref[PAIRS.index((k, s))] = split(total)


def merge(odd, mine, other, keep, got):
    n = mine.shape[1]
    half = keep.shape[0]
    vmem = pl.BlockSpec(memory_space=pltpu.VMEM)
    wide = jax.ShapeDtypeStruct((half, 3 * n), jnp.float32)
    return pl.pallas_call(
        merge_body,
        out_shape=(
            jax.ShapeDtypeStruct((6, n, n), jnp.bfloat16),
            jax.ShapeDtypeStruct((6, n, n), jnp.bfloat16),
            wide,
            jax.ShapeDtypeStruct((3 * n, 3 * n), jnp.float32),
            wide,
        ),
        in_specs=[pl.BlockSpec(memory_space=pltpu.SMEM)] + [vmem] * 4,
        out_specs=(vmem,) * 5,
        compiler_params=pltpu.CompilerParams(vmem_limit_bytes=48 * 1024 * 1024),
        interpret=INTERPRET,
        name="merge",
    )(odd, mine, other, keep, got)


def hop_body(where_ref, state_ref, high_ref, low_ref, add_ref, out_ref):
    n = high_ref.shape[1]

    @pl.when(where_ref[0] == where_ref[1])
    def _():
        high, low = split(state_ref[...])
        count = high.shape[0]
        both = jnp.concatenate([high, low], axis=0)
        for s in range(3):
            total = add_ref[:, s * n : (s + 1) * n]
            for k in range(s + 1):
                at = PAIRS.index((k, s))
                columns = slice(k * n, (k + 1) * n)
                main = lax.dot_general(both[:, columns], high_ref[at], NN, preferred_element_type=jnp.float32)
                side = lax.dot_general(high[:, columns], low_ref[at], NN, preferred_element_type=jnp.float32)
                total = total + (main[:count] + (main[count:] + side))
            out_ref[:, s * n : (s + 1) * n] = total

    @pl.when(where_ref[0] != where_ref[1])
    def _():
        out_ref[...] = jnp.zeros(out_ref.shape, jnp.float32)


def hop_on(where, state, high, low, add):
    vmem = pl.BlockSpec(memory_space=pltpu.VMEM)
    return pl.pallas_call(
        hop_body,
        out_shape=jax.ShapeDtypeStruct(state.shape, jnp.float32),
        in_specs=[pl.BlockSpec(memory_space=pltpu.SMEM)] + [vmem] * 4,
        out_specs=vmem,
        compiler_params=pltpu.CompilerParams(vmem_limit_bytes=16 * 1024 * 1024),
        interpret=INTERPRET,
        name="hop",
    )(where, state, high, low, add)


def product(left, right):
    return jnp.dot(left, right, precision=lax.Precision.HIGH, preferred_element_type=jnp.float32)


def ring(value, axis, step):
    count = lax.axis_size(axis)
    return lax.ppermute(value, axis, [(k, (k + step) % count) for k in range(count)])


def from_next(value):
    count = lax.axis_size(ROW)
    return lax.ppermute(value, ROW, [(k + 1, k) for k in range(count - 1)])


def gather_near(value):
    before = ring(value, "zh", 1)
    after = ring(value, "zh", -1)
    far = ring(before, "zh", 1)
    return jnp.concatenate([value, after, far, before], axis=1)


def shards(eigenvectors, householder):
    position = lax.axis_index(ROW)
    count = lax.axis_size(ROW)
    is_first = position == 0
    is_last = position == count - 1
    is_odd = lax.axis_index("core") == 1
    n = eigenvectors.shape[0] // 2
    local = jnp.swapaxes(householder, 2, 3)
    moved = from_next(jnp.concatenate([local[0], local[1, :1]], axis=0))
    stay = jnp.stack([jnp.where(is_first, local[0, 1], local[2, 0]), local[2, 1], local[1, 1]])
    at = [lax.axis_index("y"), lax.axis_index("zh")]
    half = 2 * moved.shape[1]

    def index(valid):
        return jnp.stack([*at, valid]).astype(jnp.int32)

    near_a = gather_near(stay)
    before_a = ring(near_a, "y", 1)
    after_a = ring(near_a, "y", -1)
    near_b = gather_near(moved)
    far0_a = ring(before_a[:, :half], "y", 1)
    far1_a = ring(after_a[:, half:], "y", -1)
    before_b = ring(near_b, "y", 1)
    after_b = ring(near_b, "y", -1)
    parts_a = prepare(index(jnp.int32(1)), near_a, after_a, before_a, far0_a, far1_a)
    before_b, after_b, parts_a = lax.optimization_barrier((before_b, after_b, parts_a))
    far0_b = ring(before_b[:, :half], "y", 1)
    far1_b = ring(after_b[:, half:], "y", -1)
    present = jnp.where(is_last, 0, 1)
    parts_b = prepare(index(present), near_b, after_b, before_b, far0_b, far1_b)
    data = from_next(eigenvectors)
    first = is_first.astype(jnp.int32).reshape(1)
    step, rest, add = operate(first, data.T, eigenvectors.T, (*parts_a, *parts_b))

    swap = [(0, 1), (1, 0)]
    half = add.shape[0] // 2
    halves = add[:, : 3 * n].reshape(2, half, 3 * n)
    keep = jnp.where(is_odd, halves[1], halves[0])
    give = jnp.where(is_odd, halves[0], halves[1])
    other = lax.ppermute(step, "core", swap)
    got = lax.ppermute(give, "core", swap)
    odd = is_odd.astype(jnp.int32).reshape(1)
    high, low, chip_add, even_step, even_add = merge(odd, step, other, keep, got)

    chips = lax.axis_size(CHIP)
    chip = lax.axis_index(CHIP)
    sub = half // SUBS
    adds = [chip_add[k * sub : (k + 1) * sub] for k in range(SUBS)]
    arrived = [[] for _ in range(SUBS)]
    for hop in range(1, chips):
        where = jnp.stack([chip, jnp.int32(hop - 1)]).astype(jnp.int32)
        for k in range(SUBS):
            sent = adds[k] if hop == 1 else hop_on(where, arrived[k][-1], high, low, adds[k])
            arrived[k].append(lax.ppermute(sent, CHIP, [(hop - 1, hop)]))
    state = jnp.concatenate([sum(values[1:], values[0]) for values in arrived], axis=0)
    odd_state = product(state, even_step) + even_add
    got = lax.ppermute(jnp.where(is_odd, state, odd_state), "core", swap)
    state = jnp.where(
        is_odd, jnp.concatenate([got, odd_state], axis=0), jnp.concatenate([state, got], axis=0)
    )
    final = product(state, rest) + add[:, 2 * n :]
    handed = from_next(final[:, n : 2 * n])
    lower = jnp.where(is_last, final[:, :n], handed)
    return jnp.concatenate([final[:, 2 * n :], lower], axis=1).T


def solution(mesh):
    split_mesh = Mesh(mesh.devices.reshape(2, 4, 2, 4, 4), (*ROW, *COL))
    return jax.shard_map(
        shards,
        mesh=split_mesh,
        in_specs=(P(ROW, COL), P(None, ROW, None, COL)),
        out_specs=P(ROW, COL),
        check_vma=False,
    )
```

```python
import jax
import jax.numpy as jnp
from jax import lax
from jax.experimental import pallas as pl
from jax.experimental.pallas import tpu as pltpu
from jax.sharding import Mesh
from jax.sharding import PartitionSpec as P

ROW = ("zl", "x", "core")
CHIP = ("zl", "x")
COL = ("y", "zh")
SUBS = 2
INTERPRET = False

NN = (((1,), (0,)), ((), ()))
NT = (((1,), (1,)), ((), ()))
TN = (((0,), (0,)), ((), ()))


def split(value):
    high = value.astype(jnp.bfloat16)
    low = (value - high.astype(jnp.float32)).astype(jnp.bfloat16)
    return high, low


def dot3(left, right, dims=NN):
    (on_left,), (on_right,) = dims[0]
    long_left = jnp.concatenate([left[0], left[0], left[1]], axis=on_left)
    long_right = jnp.concatenate([right[0], right[1], right[0]], axis=on_right)
    return lax.dot_general(long_left, long_right, dims, preferred_element_type=jnp.float32)


def prepare_body(index_ref, near_ref, after_ref, before_ref, far0_ref, far1_ref, high_ref, low_ref, v_ref, g_ref, p_ref):
    blocks, quarter, m = near_ref.shape
    n = 4 * quarter
    half = n // 2
    piece = quarter // 4
    at_y = index_ref[0]
    at_z = index_ref[1]
    valid = index_ref[2] == 1
    for block in range(blocks):
        for dy in range(4):
            base = lax.rem(at_y + dy, 4) * quarter
            for dz in range(4):
                start = base + lax.rem(at_z + dz, 4) * piece
                at = pl.ds(dz * piece, piece)
                if dy == 0:
                    part = near_ref[block, at, :]
                elif dy == 1:
                    part = after_ref[block, at, :]
                elif dy == 3:
                    part = before_ref[block, at, :]
                elif dz < 2:
                    part = far0_ref[block, at, :]
                else:
                    part = far1_ref[block, pl.ds((dz - 2) * piece, piece), :]
                v_ref[block, pl.ds(start, piece), :] = part
    rows = lax.broadcasted_iota(jnp.int32, (half, half), 0)
    cols = lax.broadcasted_iota(jnp.int32, (half, half), 1)
    eye = rows == cols
    pair = (rows // 2 == cols // 2) & (rows < cols)
    for block in range(blocks):
        vectors = split(v_ref[block])
        g_ref[block] = dot3(vectors, vectors, NT)
    problems = [(block, side) for block in range(blocks) for side in range(2)]
    for at, (block, side) in enumerate(problems):
        lo = side * half
        gram = g_ref[block, lo : lo + half, lo : lo + half]
        on_diagonal = jnp.where(eye, gram, 0.0)
        col_inverse = 1.0 / (0.5 * jnp.sum(on_diagonal, axis=1, keepdims=True))
        row_inverse = 1.0 / (0.5 * jnp.sum(on_diagonal, axis=0, keepdims=True))
        inverse = jnp.where(eye, col_inverse, 0.0)
        p_ref[at] = inverse - jnp.where(pair, gram * col_inverse * row_inverse, 0.0)

    levels = half.bit_length() - 1

    def level(power, carry):
        old_rows = jnp.right_shift(rows, power)
        old_cols = jnp.right_shift(cols, power)
        corner = (jnp.right_shift(old_rows, 1) == jnp.right_shift(old_cols, 1)) & (old_rows < old_cols)
        first = []
        for at, (block, side) in enumerate(problems):
            lo = side * half
            edge = split(jnp.where(corner, g_ref[block, lo : lo + half, lo : lo + half], 0.0))
            first.append(dot3(split(p_ref[at]), edge))
        for at in range(len(problems)):
            old = p_ref[at]
            p_ref[at] = old - dot3(split(first[at]), split(old))
        return carry

    lax.fori_loop(1, levels, level, 0)
    eye = lax.broadcasted_iota(jnp.int32, (m, m), 0) == lax.broadcasted_iota(jnp.int32, (m, m), 1)
    unit = jnp.where(eye, 1.0, 0.0)
    first = [
        dot3(split(p_ref[2 * block]), split(g_ref[block, :half, half:])) for block in range(blocks)
    ]
    corners = [dot3(split(first[block]), split(p_ref[2 * block + 1])) for block in range(blocks)]
    for block in range(blocks):
        vectors = split(v_ref[block])
        top = split(jnp.concatenate([p_ref[2 * block], -corners[block]], axis=1))
        low = split(p_ref[2 * block + 1])
        upper = dot3(top, vectors)
        lower = dot3(low, (vectors[0][half:], vectors[1][half:]))
        scaled = split(jnp.concatenate([upper, lower], axis=0).T)
        whole = unit - dot3(scaled, vectors)
        whole = jnp.where(valid, whole, unit)
        high, low = split(whole)
        high_ref[block] = high
        low_ref[block] = low


def prepare(index, near, after, before, far0, far1):
    blocks, quarter, m = near.shape
    n = 4 * quarter
    out = jax.ShapeDtypeStruct((blocks, m, m), jnp.bfloat16)
    vmem = pl.BlockSpec(memory_space=pltpu.VMEM)
    return pl.pallas_call(
        prepare_body,
        out_shape=(out, out),
        in_specs=[pl.BlockSpec(memory_space=pltpu.SMEM)] + [vmem] * 5,
        out_specs=(vmem, vmem),
        scratch_shapes=[
            pltpu.VMEM((blocks, n, m), jnp.float32),
            pltpu.VMEM((blocks, n, n), jnp.float32),
            pltpu.VMEM((2 * blocks, n // 2, n // 2), jnp.float32),
        ],
        compiler_params=pltpu.CompilerParams(vmem_limit_bytes=14 * 1024 * 1024),
        cost_estimate=pl.CostEstimate(flops=2_000_000_000, bytes_accessed=1_000_000, transcendentals=0),
        interpret=INTERPRET,
        name="prepare",
    )(index, near, after, before, far0, far1)


PAIRS = ((0, 0), (0, 1), (0, 2), (1, 1), (1, 2), (2, 2))


def operate_body(first_ref, data_ref, own_ref, ah, al, bh, bl, step_ref, rest_ref, add_ref):
    n = ah.shape[1] // 2
    first = first_ref[0] == 1
    width = data_ref.shape[0]
    where_held = {(0, 0): (bh, bl, 0), (0, 1): (bh, bl, 1), (1, 0): (ah, al, 2), (1, 1): (bh, bl, 2), (2, 0): (ah, al, 0), (2, 1): (ah, al, 1)}

    def part(sweep, block, side=None):
        high, low, at = where_held[sweep, block]
        if side is None:
            return high[at], low[at]
        rows = pl.ds(side * n, n)
        return high[at, rows, :], low[at, rows, :]

    extra = dot3(split(own_ref[...]), part(2, 0))
    own = data_ref[...]
    start = jnp.where(first, extra, 0.0)
    incoming = (start[:, n:], start[:, :n], jnp.zeros((width, n), jnp.float32))
    for sweep in range(3):
        a = part(sweep, 0)
        if sweep == 2:
            size = 2 * n
            eye = lax.broadcasted_iota(jnp.int32, (size, size), 0) == lax.broadcasted_iota(jnp.int32, (size, size), 1)
            a = (
                jnp.where(first, eye.astype(jnp.float32), a[0].astype(jnp.float32)).astype(jnp.bfloat16),
                jnp.where(first, 0.0, a[1].astype(jnp.float32)).astype(jnp.bfloat16),
            )
        a_top = (a[0][:n], a[1][:n])
        a_low = (a[0][n:], a[1][n:])
        b_top = part(sweep, 1, 0)
        b_low = part(sweep, 1, 1)
        fresh = a_top[0].astype(jnp.float32) + a_top[1].astype(jnp.float32)
        if sweep == 0:
            u, v = own[:, :n], own[:, n:]
            mid = dot3(split(jnp.concatenate([incoming[0], u], axis=1)), a)
            mid = jnp.concatenate([fresh, mid], axis=0)
            done = dot3(split(mid[:, n:]), b_top)
            last = dot3(split(v), b_low)
            done = jnp.concatenate([done[:n], done[n:] + last], axis=0)
        else:
            mid = dot3(split(u), a_low)
            if sweep == 1:
                data = mid[-width:] + dot3(split(incoming[sweep]), a_top)
                mid = jnp.concatenate([mid[:-width], fresh, data], axis=0)
            else:
                mid = jnp.concatenate([mid[:-width], fresh, mid[-width:]], axis=0)
            done = dot3(split(mid[:, n:]), b_top)
            last = dot3(split(v), b_low)
            early = sweep * n
            done = jnp.concatenate(
                [done[:early] + last[:early], done[early : early + n], done[early + n :] + last[early:]], axis=0
            )
        known = (sweep + 1) * n
        u, v = mid[:, :n], done[:, :n]
        out = done[:, n:]
        for k in range(sweep + 1):
            step_ref[PAIRS.index((k, sweep))] = out[k * n : (k + 1) * n]
        add_ref[:, sweep * n : (sweep + 1) * n] = out[known:]
    rest_ref[:, 0:n] = out[: 3 * n]
    rest_ref[:, n : 2 * n] = u[: 3 * n]
    rest_ref[:, 2 * n : 3 * n] = v[: 3 * n]
    add_ref[:, 3 * n : 4 * n] = u[3 * n :]
    add_ref[:, 4 * n : 5 * n] = v[3 * n :]


def operate(first, data, own, parts):
    width, m = data.shape
    n = m // 2
    vmem = pl.BlockSpec(memory_space=pltpu.VMEM)
    return pl.pallas_call(
        operate_body,
        out_shape=(
            jax.ShapeDtypeStruct((6, n, n), jnp.float32),
            jax.ShapeDtypeStruct((3 * n, 3 * n), jnp.float32),
            jax.ShapeDtypeStruct((width, 5 * n), jnp.float32),
        ),
        in_specs=[pl.BlockSpec(memory_space=pltpu.SMEM)] + [vmem] * 6,
        out_specs=(vmem,) * 3,
        compiler_params=pltpu.CompilerParams(vmem_limit_bytes=20 * 1024 * 1024),
        interpret=INTERPRET,
        name="operate",
    )(first, data, own, *parts)


def merge_body(odd_ref, mine_ref, other_ref, keep_ref, got_ref, high_ref, low_ref, add_ref):
    n = mine_ref.shape[1]
    odd = odd_ref[0] == 1
    keep = keep_ref[...]
    got = got_ref[...]
    even_parts = [split(jnp.where(odd, other_ref[k], mine_ref[k])) for k in range(6)]
    odd_parts = [split(jnp.where(odd, mine_ref[k], other_ref[k])) for k in range(6)]
    odd_add = jnp.where(odd, keep, got)
    add_parts = split(jnp.where(odd, got, keep))
    for s in range(3):
        total = odd_add[:, s * n : (s + 1) * n]
        for j in range(s + 1):
            columns = slice(j * n, (j + 1) * n)
            total = total + dot3((add_parts[0][:, columns], add_parts[1][:, columns]), odd_parts[PAIRS.index((j, s))])
        add_ref[:, s * n : (s + 1) * n] = total
        for k in range(s + 1):
            total = None
            for j in range(k, s + 1):
                term = dot3(even_parts[PAIRS.index((k, j))], odd_parts[PAIRS.index((j, s))])
                total = term if total is None else total + term
            high_ref[PAIRS.index((k, s))], low_ref[PAIRS.index((k, s))] = split(total)


def merge(odd, mine, other, keep, got):
    n = mine.shape[1]
    half = keep.shape[0]
    vmem = pl.BlockSpec(memory_space=pltpu.VMEM)
    packed = jax.ShapeDtypeStruct((6, n, n), jnp.bfloat16)
    return pl.pallas_call(
        merge_body,
        out_shape=(packed, packed, jax.ShapeDtypeStruct((half, 3 * n), jnp.float32)),
        in_specs=[pl.BlockSpec(memory_space=pltpu.SMEM)] + [vmem] * 4,
        out_specs=(vmem,) * 3,
        compiler_params=pltpu.CompilerParams(vmem_limit_bytes=20 * 1024 * 1024),
        interpret=INTERPRET,
        name="merge",
    )(odd, mine, other, keep, got)


def hop_body(state_ref, high_ref, low_ref, add_ref, out_ref):
    n = high_ref.shape[1]
    high, low = split(state_ref[...])
    count = high.shape[0]
    both = jnp.concatenate([high, low], axis=0)
    for s in range(3):
        total = add_ref[:, s * n : (s + 1) * n]
        for k in range(s + 1):
            at = PAIRS.index((k, s))
            columns = slice(k * n, (k + 1) * n)
            main = lax.dot_general(both[:, columns], high_ref[at], NN, preferred_element_type=jnp.float32)
            side = lax.dot_general(high[:, columns], low_ref[at], NN, preferred_element_type=jnp.float32)
            total = total + (main[:count] + (main[count:] + side))
        out_ref[:, s * n : (s + 1) * n] = total


def hop_on(state, high, low, add):
    vmem = pl.BlockSpec(memory_space=pltpu.VMEM)
    return pl.pallas_call(
        hop_body,
        out_shape=jax.ShapeDtypeStruct(state.shape, jnp.float32),
        in_specs=[vmem] * 4,
        out_specs=vmem,
        compiler_params=pltpu.CompilerParams(vmem_limit_bytes=8 * 1024 * 1024),
        interpret=INTERPRET,
        name="hop",
    )(state, high, low, add)


def ending_body(odd_ref, mine_ref, other_ref, rest_ref, other_rest_ref, keep_ref, got_ref, high_ref, low_ref, add_ref):
    n = mine_ref.shape[1]
    odd = odd_ref[0] == 1
    for k in range(3):
        rows = slice(k * n, (k + 1) * n)
        even_rest = jnp.where(odd, other_rest_ref[rows, n:], rest_ref[rows, n:])
        high_ref[rows, : 2 * n], low_ref[rows, : 2 * n] = split(even_rest)
    odd_parts = []
    for k in range(3):
        rows = slice(k * n, (k + 1) * n)
        odd_parts.append(split(jnp.where(odd, rest_ref[rows, :], other_rest_ref[rows, :])))
    for k in range(3):
        total = None
        for j in range(k, 3):
            at = PAIRS.index((k, j))
            term = dot3(split(jnp.where(odd, other_ref[at], mine_ref[at])), odd_parts[j])
            total = term if total is None else total + term
        rows = slice(k * n, (k + 1) * n)
        high_ref[rows, 2 * n :], low_ref[rows, 2 * n :] = split(total)
    even_add = jnp.where(odd, got_ref[...], keep_ref[...])
    odd_add = jnp.where(odd, keep_ref[...], got_ref[...])
    total = odd_add[:, 2 * n :]
    for j in range(3):
        total = total + dot3(split(even_add[:, j * n : (j + 1) * n]), odd_parts[j])
    add_ref[:, : 2 * n] = even_add[:, 3 * n :]
    add_ref[:, 2 * n :] = total


def ending(odd, mine, other, rest, other_rest, keep, got):
    n = mine.shape[1]
    vmem = pl.BlockSpec(memory_space=pltpu.VMEM)
    wide = jax.ShapeDtypeStruct((3 * n, 5 * n), jnp.bfloat16)
    return pl.pallas_call(
        ending_body,
        out_shape=(wide, wide, jax.ShapeDtypeStruct(keep.shape, jnp.float32)),
        in_specs=[pl.BlockSpec(memory_space=pltpu.SMEM)] + [vmem] * 6,
        out_specs=(vmem,) * 3,
        compiler_params=pltpu.CompilerParams(vmem_limit_bytes=16 * 1024 * 1024),
        interpret=INTERPRET,
        name="ending",
    )(odd, mine, other, rest, other_rest, keep, got)


def finish_body(*refs):
    *state_refs, high_ref, low_ref, add_ref, out_ref = refs
    hops = len(state_refs) // SUBS
    rows = []
    for k in range(SUBS):
        total = state_refs[k * hops][...]
        for ref in state_refs[k * hops + 1 : (k + 1) * hops]:
            total = total + ref[...]
        rows.append(total)
    state = split(jnp.concatenate(rows, axis=0))
    out_ref[...] = dot3(state, (high_ref[...], low_ref[...])) + add_ref[...]


def finish(arrived, high, low, add):
    vmem = pl.BlockSpec(memory_space=pltpu.VMEM)
    states = [value for values in arrived for value in values]
    return pl.pallas_call(
        finish_body,
        out_shape=jax.ShapeDtypeStruct(add.shape, jnp.float32),
        in_specs=[vmem] * (len(states) + 3),
        out_specs=vmem,
        compiler_params=pltpu.CompilerParams(vmem_limit_bytes=16 * 1024 * 1024),
        interpret=INTERPRET,
        name="finish",
    )(*states, high, low, add)


def ring(value, axis, step):
    count = lax.axis_size(axis)
    return lax.ppermute(value, axis, [(k, (k + step) % count) for k in range(count)])


def from_next(value):
    count = lax.axis_size(ROW)
    return lax.ppermute(value, ROW, [(k + 1, k) for k in range(count - 1)])


def gather_near(value):
    before = ring(value, "zh", 1)
    after = ring(value, "zh", -1)
    far = ring(before, "zh", 1)
    return jnp.concatenate([value, after, far, before], axis=1)


def shards(eigenvectors, householder):
    local = jnp.swapaxes(householder, 2, 3)
    position = lax.axis_index(ROW)
    count = lax.axis_size(ROW)
    chips = lax.axis_size(CHIP)
    is_first = position == 0
    is_last = position == count - 1
    is_odd = lax.axis_index("core") == 1
    on_last = lax.axis_index(CHIP) == chips - 1
    inner_odd = is_odd & jnp.logical_not(on_last)
    at = [lax.axis_index("y"), lax.axis_index("zh")]
    index_a = jnp.stack([*at, jnp.int32(1)]).astype(jnp.int32)
    index_b = jnp.stack([*at, jnp.where(is_last, 0, 1)]).astype(jnp.int32)
    first = is_first.astype(jnp.int32).reshape(1)
    odd = is_odd.astype(jnp.int32).reshape(1)
    local, is_first, is_odd, on_last, inner_odd, index_a, index_b, first, odd = lax.optimization_barrier(
        (local, is_first, is_odd, on_last, inner_odd, index_a, index_b, first, odd)
    )
    n = eigenvectors.shape[0] // 2
    blocks, piece, m = local.shape[1] + 1, local.shape[2], local.shape[3]
    mine = eigenvectors.T
    leaving = jnp.concatenate([local[0], local[1, :1]], axis=0).reshape(blocks * piece, m)
    moved = from_next(jnp.concatenate([leaving, mine], axis=0))
    data = moved[blocks * piece :]
    moved = moved[: blocks * piece].reshape(blocks, piece, m)
    stay = jnp.stack([jnp.where(is_first, local[0, 1], local[2, 0]), local[2, 1], local[1, 1]])
    half = 2 * piece
    near_a = gather_near(stay)
    before_a = ring(near_a, "y", 1)
    after_a = ring(near_a, "y", -1)
    near_b = gather_near(moved)
    far0_a = ring(before_a[:, :half], "y", 1)
    far1_a = ring(after_a[:, half:], "y", -1)
    before_b = ring(near_b, "y", 1)
    after_b = ring(near_b, "y", -1)
    parts_a = prepare(index_a, near_a, after_a, before_a, far0_a, far1_a)
    before_b, after_b, parts_a = lax.optimization_barrier((before_b, after_b, parts_a))
    far0_b = ring(before_b[:, :half], "y", 1)
    far1_b = ring(after_b[:, half:], "y", -1)
    parts_b = prepare(index_b, near_b, after_b, before_b, far0_b, far1_b)
    step, rest, add = operate(first, data, mine, (*parts_a, *parts_b))

    swap = [(0, 1), (1, 0)]
    half = add.shape[0] // 2
    halves = add.reshape(2, half, 5 * n)
    keep = jnp.where(is_odd, halves[1], halves[0])
    give = jnp.where(is_odd, halves[0], halves[1])
    other = lax.ppermute(step, "core", swap)
    got = lax.ppermute(give, "core", swap)
    rest, other, got = lax.optimization_barrier((rest, other, got))
    high, low, chip_add = merge(odd, step, other, keep[:, : 3 * n], got[:, : 3 * n])
    other_rest = lax.ppermute(rest, "core", swap)

    sub = half // SUBS
    adds = [chip_add[k * sub : (k + 1) * sub] for k in range(SUBS)]
    arrived = [[lax.ppermute(part, CHIP, [(0, 1)])] for part in adds]

    rest_high, rest_low, rest_add = ending(odd, step, other, rest, other_rest, keep, got)
    arrived[0][0], arrived[1][0], rest_high, rest_low, rest_add = lax.optimization_barrier(
        (arrived[0][0], arrived[1][0], rest_high, rest_low, rest_add)
    )
    for hop in range(2, chips):
        for k in range(SUBS):
            sent = hop_on(arrived[k][-1], high, low, adds[k])
            arrived[k].append(lax.ppermute(sent, CHIP, [(hop - 1, hop)]))
    final = finish(arrived, rest_high, rest_low, rest_add)
    even_top, even_low, odd_end, odd_top, odd_low = [final[:, k * n : (k + 1) * n] for k in range(5)]
    for_even = jnp.concatenate([even_low, odd_top], axis=1)
    for_odd = jnp.concatenate([odd_low, odd_end], axis=1)
    got = lax.ppermute(jnp.where(is_odd, for_even, for_odd), "core", swap)
    chip_rows = [(2 * k, 2 * k + 1) for k in range(chips)]
    handed = [
        lax.ppermute(even_top, ROW, [(chip_rows[k + 1][side], chip_rows[k][1]) for k in range(chips - 1)])
        for side in range(2)
    ]
    got, *handed = lax.optimization_barrier((got, *handed))
    theirs = jnp.where(inner_odd, jnp.concatenate([got[:, :n], handed[0]], axis=1), got)
    tail = jnp.where(on_last, odd_end, handed[1])
    ours = jnp.where(is_odd, jnp.concatenate([odd_low, tail], axis=1), for_even)
    upper = jnp.where(is_odd, theirs, ours)
    lower = jnp.where(is_odd, ours, theirs)
    return jnp.concatenate([upper, lower], axis=0).T


def solution(mesh):
    split_mesh = Mesh(mesh.devices.reshape(2, 4, 2, 4, 4), (*ROW, *COL))
    return jax.shard_map(
        shards,
        mesh=split_mesh,
        in_specs=(P(ROW, COL), P(None, ROW, None, COL)),
        out_specs=P(ROW, COL),
        check_vma=False,
    )
```

```python
import functools

import jax
import jax.numpy as jnp
from jax import lax
from jax.experimental import pallas as pl
from jax.experimental.pallas import tpu as pltpu
from jax.sharding import Mesh
from jax.sharding import PartitionSpec as P

ROW = ("zl", "x", "core")
CHIP = ("zl", "x")
COL = ("y", "zh")
SUBS = 2
INTERPRET = False

NN = (((1,), (0,)), ((), ()))
NT = (((1,), (1,)), ((), ()))
TN = (((0,), (0,)), ((), ()))


def split(value):
    high = value.astype(jnp.bfloat16)
    low = (value - high.astype(jnp.float32)).astype(jnp.bfloat16)
    return high, low


def dot3(left, right, dims=NN):
    (on_left,), (on_right,) = dims[0]
    long_left = jnp.concatenate([left[0], left[0], left[1]], axis=on_left)
    long_right = jnp.concatenate([right[0], right[1], right[0]], axis=on_right)
    return lax.dot_general(long_left, long_right, dims, preferred_element_type=jnp.float32)


def prepare_body(outer_y, index_ref, near_ref, after_ref, before_ref, far0_ref, far1_ref, high_ref, low_ref, v_ref, g_ref, p_ref):
    blocks, quarter, m = near_ref.shape
    n = 4 * quarter
    half = n // 2
    piece = quarter // 4
    at_y = index_ref[0]
    at_z = index_ref[1]
    for outer in range(4):
        for inner in range(4):
            dy, dz = (outer, inner) if outer_y else (inner, outer)
            start = lax.rem(at_y + dy, 4) * quarter + lax.rem(at_z + dz, 4) * piece
            at = pl.ds(inner * piece, piece)
            for block in range(blocks):
                if outer == 0:
                    part = near_ref[block, at, :]
                elif outer == 1:
                    part = after_ref[block, at, :]
                elif outer == 3:
                    part = before_ref[block, at, :]
                elif inner < 2:
                    part = far0_ref[block, at, :]
                else:
                    part = far1_ref[block, pl.ds((inner - 2) * piece, piece), :]
                v_ref[block, pl.ds(start, piece), :] = part
    rows = lax.broadcasted_iota(jnp.int32, (half, half), 0)
    cols = lax.broadcasted_iota(jnp.int32, (half, half), 1)
    eye = rows == cols
    pair = (rows // 2 == cols // 2) & (rows < cols)
    for block in range(blocks):
        vectors = split(v_ref[block])
        g_ref[block] = dot3(vectors, vectors, NT)
    problems = [(block, side) for block in range(blocks) for side in range(2)]
    for at, (block, side) in enumerate(problems):
        lo = side * half
        gram = g_ref[block, lo : lo + half, lo : lo + half]
        on_diagonal = jnp.where(eye, gram, 0.0)
        col_inverse = 1.0 / (0.5 * jnp.sum(on_diagonal, axis=1, keepdims=True))
        row_inverse = 1.0 / (0.5 * jnp.sum(on_diagonal, axis=0, keepdims=True))
        inverse = jnp.where(eye, col_inverse, 0.0)
        p_ref[at] = inverse - jnp.where(pair, gram * col_inverse * row_inverse, 0.0)

    levels = half.bit_length() - 1

    def level(power, carry):
        old_rows = jnp.right_shift(rows, power)
        old_cols = jnp.right_shift(cols, power)
        corner = (jnp.right_shift(old_rows, 1) == jnp.right_shift(old_cols, 1)) & (old_rows < old_cols)
        first = []
        for at, (block, side) in enumerate(problems):
            lo = side * half
            edge = split(jnp.where(corner, g_ref[block, lo : lo + half, lo : lo + half], 0.0))
            first.append(dot3(split(p_ref[at]), edge))
        for at in range(len(problems)):
            old = p_ref[at]
            p_ref[at] = old - dot3(split(first[at]), split(old))
        return carry

    lax.fori_loop(1, levels, level, 0)
    eye = lax.broadcasted_iota(jnp.int32, (m, m), 0) == lax.broadcasted_iota(jnp.int32, (m, m), 1)
    unit = jnp.where(eye, 1.0, 0.0)
    first = [
        dot3(split(p_ref[2 * block]), split(g_ref[block, :half, half:])) for block in range(blocks)
    ]
    corners = [dot3(split(first[block]), split(p_ref[2 * block + 1])) for block in range(blocks)]
    for block in range(blocks):
        vectors = split(v_ref[block])
        top = split(jnp.concatenate([p_ref[2 * block], -corners[block]], axis=1))
        low = split(p_ref[2 * block + 1])
        upper = dot3(top, vectors)
        lower = dot3(low, (vectors[0][half:], vectors[1][half:]))
        scaled = split(jnp.concatenate([upper, lower], axis=0).T)
        whole = unit - dot3(scaled, vectors)
        whole = jnp.where(index_ref[2 + block] == 1, whole, unit)
        high, low = split(whole)
        high_ref[block] = high
        low_ref[block] = low


def prepare(outer_y, index, near, after, before, far0, far1):
    blocks, quarter, m = near.shape
    n = 4 * quarter
    out = jax.ShapeDtypeStruct((blocks, m, m), jnp.bfloat16)
    vmem = pl.BlockSpec(memory_space=pltpu.VMEM)
    return pl.pallas_call(
        functools.partial(prepare_body, outer_y),
        out_shape=(out, out),
        in_specs=[pl.BlockSpec(memory_space=pltpu.SMEM)] + [vmem] * 5,
        out_specs=(vmem, vmem),
        scratch_shapes=[
            pltpu.VMEM((blocks, n, m), jnp.float32),
            pltpu.VMEM((blocks, n, n), jnp.float32),
            pltpu.VMEM((2 * blocks, n // 2, n // 2), jnp.float32),
        ],
        compiler_params=pltpu.CompilerParams(vmem_limit_bytes=14 * 1024 * 1024),
        cost_estimate=pl.CostEstimate(flops=2_000_000_000, bytes_accessed=1_000_000, transcendentals=0),
        interpret=INTERPRET,
        name="prepare",
    )(index, near, after, before, far0, far1)


PAIRS = ((0, 0), (0, 1), (0, 2), (1, 1), (1, 2), (2, 2))


def operate_body(ends_ref, data_ref, own_ref, ah, al, bh, bl, step_ref, rest_ref, add_ref):
    n = ah.shape[1] // 2
    first = ends_ref[0] == 1
    last = ends_ref[1] == 1
    width = data_ref.shape[0]
    held = {(0, 0): (ah, al, 0), (0, 1): (bh, bl, 0), (1, 0): (ah, al, 1), (1, 1): (ah, al, 2), (2, 0): (bh, bl, 1), (2, 1): (ah, al, 3)}

    def part(sweep, block, side=None):
        high, low, at = held[sweep, block]
        if side is None:
            return high[at], low[at]
        rows = pl.ds(side * n, n)
        return high[at, rows, :], low[at, rows, :]

    outs = []
    for sweep in range(3):
        a_top = part(sweep, 0, 0)
        b_top = part(sweep, 1, 0)
        b_low = part(sweep, 1, 1)
        fresh = a_top[0].astype(jnp.float32) + a_top[1].astype(jnp.float32)
        if sweep == 0:
            own = own_ref[...]
            arriving = jnp.where(first, own[:, :n], 0.0)
            mid = dot3(split(jnp.concatenate([arriving, own[:, n:]], axis=1)), part(0, 0))
            mid = jnp.concatenate([fresh, mid], axis=0)
            v = data_ref[...]
            done = dot3(split(mid[:, n:]), b_top)
            done = jnp.concatenate([done[:n], done[n:] + dot3(split(v), b_low)], axis=0)
            v = jnp.concatenate([jnp.zeros((n, n), jnp.float32), v], axis=0)
            done = jnp.where(last, jnp.concatenate([mid[:, n:], v], axis=1), done)
        else:
            mid = dot3(split(u), part(sweep, 0, 1))
            mid = jnp.concatenate([mid[:-width], fresh, mid[-width:]], axis=0)
            done = dot3(split(mid[:, n:]), b_top)
            more = dot3(split(v), b_low)
            early = sweep * n
            done = jnp.concatenate(
                [done[:early] + more[:early], done[early : early + n], done[early + n :] + more[early:]], axis=0
            )
        known = (sweep + 1) * n
        u, v = mid[:, :n], done[:, :n]
        out = done[:, n:]
        for k in range(sweep + 1):
            step_ref[PAIRS.index((k, sweep))] = out[k * n : (k + 1) * n]
        add_ref[:, sweep * n : (sweep + 1) * n] = out[known:]
    rest_ref[:, 0:n] = u[: 3 * n]
    rest_ref[:, n : 2 * n] = v[: 3 * n]
    add_ref[:, 3 * n : 4 * n] = u[3 * n :]
    add_ref[:, 4 * n : 5 * n] = v[3 * n :]

    @pl.when(last)
    def _():
        high, low = bh[0], bl[0]
        for k in range(4):
            if k < 3:
                upper = step_ref[PAIRS.index((k, 2))]
                lower = step_ref[PAIRS.index((k, 1))] if k < 2 else jnp.zeros((n, n), jnp.float32)
            else:
                upper = add_ref[:, 2 * n : 3 * n]
                lower = add_ref[:, n : 2 * n]
            result = dot3(split(jnp.concatenate([upper, lower], axis=1)), (high, low))
            if k < 3:
                rest_ref[k * n : (k + 1) * n, 2 * n :] = result
            else:
                add_ref[:, 5 * n :] = result

    @pl.when(jnp.logical_not(last))
    def _():
        rest_ref[:, 2 * n :] = jnp.zeros((3 * n, 2 * n), jnp.float32)
        add_ref[:, 5 * n :] = jnp.zeros((width, 2 * n), jnp.float32)


def operate(ends, data, own, parts):
    width, m = own.shape
    n = m // 2
    vmem = pl.BlockSpec(memory_space=pltpu.VMEM)
    return pl.pallas_call(
        operate_body,
        out_shape=(
            jax.ShapeDtypeStruct((6, n, n), jnp.float32),
            jax.ShapeDtypeStruct((3 * n, 4 * n), jnp.float32),
            jax.ShapeDtypeStruct((width, 7 * n), jnp.float32),
        ),
        in_specs=[pl.BlockSpec(memory_space=pltpu.SMEM)] + [vmem] * 6,
        out_specs=(vmem,) * 3,
        compiler_params=pltpu.CompilerParams(vmem_limit_bytes=20 * 1024 * 1024),
        interpret=INTERPRET,
        name="operate",
    )(ends, data, own, *parts)


def merge_body(odd_ref, mine_ref, other_ref, keep_ref, got_ref, high_ref, low_ref, add_ref):
    n = mine_ref.shape[1]
    odd = odd_ref[0] == 1
    keep = keep_ref[...]
    got = got_ref[...]
    even_parts = [split(jnp.where(odd, other_ref[k], mine_ref[k])) for k in range(6)]
    odd_parts = [split(jnp.where(odd, mine_ref[k], other_ref[k])) for k in range(6)]
    odd_add = jnp.where(odd, keep, got)
    add_parts = split(jnp.where(odd, got, keep))
    for s in range(3):
        total = odd_add[:, s * n : (s + 1) * n]
        for j in range(s + 1):
            columns = slice(j * n, (j + 1) * n)
            total = total + dot3((add_parts[0][:, columns], add_parts[1][:, columns]), odd_parts[PAIRS.index((j, s))])
        add_ref[:, s * n : (s + 1) * n] = total
        for k in range(s + 1):
            total = None
            for j in range(k, s + 1):
                term = dot3(even_parts[PAIRS.index((k, j))], odd_parts[PAIRS.index((j, s))])
                total = term if total is None else total + term
            high_ref[PAIRS.index((k, s))], low_ref[PAIRS.index((k, s))] = split(total)


def merge(odd, mine, other, keep, got):
    n = mine.shape[1]
    half = keep.shape[0]
    vmem = pl.BlockSpec(memory_space=pltpu.VMEM)
    packed = jax.ShapeDtypeStruct((6, n, n), jnp.bfloat16)
    return pl.pallas_call(
        merge_body,
        out_shape=(packed, packed, jax.ShapeDtypeStruct((half, 3 * n), jnp.float32)),
        in_specs=[pl.BlockSpec(memory_space=pltpu.SMEM)] + [vmem] * 4,
        out_specs=(vmem,) * 3,
        compiler_params=pltpu.CompilerParams(vmem_limit_bytes=20 * 1024 * 1024),
        interpret=INTERPRET,
        name="merge",
    )(odd, mine, other, keep, got)


def hop_body(state_ref, high_ref, low_ref, add_ref, out_ref):
    n = high_ref.shape[1]
    high, low = split(state_ref[...])
    count = high.shape[0]
    both = jnp.concatenate([high, low], axis=0)
    for s in range(3):
        total = add_ref[:, s * n : (s + 1) * n]
        for k in range(s + 1):
            at = PAIRS.index((k, s))
            columns = slice(k * n, (k + 1) * n)
            main = lax.dot_general(both[:, columns], high_ref[at], NN, preferred_element_type=jnp.float32)
            side = lax.dot_general(high[:, columns], low_ref[at], NN, preferred_element_type=jnp.float32)
            total = total + (main[:count] + (main[count:] + side))
        out_ref[:, s * n : (s + 1) * n] = total


def hop_on(state, high, low, add):
    vmem = pl.BlockSpec(memory_space=pltpu.VMEM)
    return pl.pallas_call(
        hop_body,
        out_shape=jax.ShapeDtypeStruct(state.shape, jnp.float32),
        in_specs=[vmem] * 4,
        out_specs=vmem,
        compiler_params=pltpu.CompilerParams(vmem_limit_bytes=8 * 1024 * 1024),
        interpret=INTERPRET,
        name="hop",
    )(state, high, low, add)


def ending_body(odd_ref, mine_ref, other_ref, rest_ref, other_rest_ref, keep_ref, got_ref, high_ref, low_ref, add_ref):
    n = mine_ref.shape[1]
    odd = odd_ref[0] == 1
    for k in range(3):
        rows = slice(k * n, (k + 1) * n)
        even_rest = jnp.where(odd, other_rest_ref[rows, : 2 * n], rest_ref[rows, : 2 * n])
        high_ref[rows, : 2 * n], low_ref[rows, : 2 * n] = split(even_rest)
    odd_parts = []
    for k in range(3):
        rows = slice(k * n, (k + 1) * n)
        odd_parts.append(split(jnp.where(odd, rest_ref[rows, :], other_rest_ref[rows, :])))
    for k in range(3):
        total = None
        for j in range(k, 3):
            at = PAIRS.index((k, j))
            term = dot3(split(jnp.where(odd, other_ref[at], mine_ref[at])), odd_parts[j])
            total = term if total is None else total + term
        rows = slice(k * n, (k + 1) * n)
        high_ref[rows, 2 * n :], low_ref[rows, 2 * n :] = split(total)
    even_add = jnp.where(odd, got_ref[...], keep_ref[...])
    odd_add = jnp.where(odd, keep_ref[...], got_ref[...])
    total = odd_add[:, 3 * n :]
    for j in range(3):
        total = total + dot3(split(even_add[:, j * n : (j + 1) * n]), odd_parts[j])
    add_ref[:, : 2 * n] = even_add[:, 3 * n : 5 * n]
    add_ref[:, 2 * n :] = total


def ending(odd, mine, other, rest, other_rest, keep, got):
    n = mine.shape[1]
    vmem = pl.BlockSpec(memory_space=pltpu.VMEM)
    wide = jax.ShapeDtypeStruct((3 * n, 6 * n), jnp.bfloat16)
    return pl.pallas_call(
        ending_body,
        out_shape=(wide, wide, jax.ShapeDtypeStruct((keep.shape[0], 6 * n), jnp.float32)),
        in_specs=[pl.BlockSpec(memory_space=pltpu.SMEM)] + [vmem] * 6,
        out_specs=(vmem,) * 3,
        compiler_params=pltpu.CompilerParams(vmem_limit_bytes=16 * 1024 * 1024),
        interpret=INTERPRET,
        name="ending",
    )(odd, mine, other, rest, other_rest, keep, got)


def finish_body(*refs):
    *state_refs, high_ref, low_ref, add_ref, out_ref = refs
    hops = len(state_refs) // SUBS
    rows = []
    for k in range(SUBS):
        total = state_refs[k * hops][...]
        for ref in state_refs[k * hops + 1 : (k + 1) * hops]:
            total = total + ref[...]
        rows.append(total)
    state = split(jnp.concatenate(rows, axis=0))
    out_ref[...] = dot3(state, (high_ref[...], low_ref[...])) + add_ref[...]


def finish(arrived, high, low, add):
    vmem = pl.BlockSpec(memory_space=pltpu.VMEM)
    states = [value for values in arrived for value in values]
    return pl.pallas_call(
        finish_body,
        out_shape=jax.ShapeDtypeStruct(add.shape, jnp.float32),
        in_specs=[vmem] * (len(states) + 3),
        out_specs=vmem,
        compiler_params=pltpu.CompilerParams(vmem_limit_bytes=16 * 1024 * 1024),
        interpret=INTERPRET,
        name="finish",
    )(*states, high, low, add)


def ring(value, axis, step):
    count = lax.axis_size(axis)
    return lax.ppermute(value, axis, [(k, (k + step) % count) for k in range(count)])


def shifted(value, step):
    count = lax.axis_size(ROW)
    return lax.ppermute(value, ROW, [(k, k + step) for k in range(max(0, -step), min(count, count - step))])


def after_these(value, others):
    return lax.optimization_barrier((value, *others))[0]


def shards(eigenvectors, householder):
    local = jnp.swapaxes(householder, 2, 3)
    position = lax.axis_index(ROW)
    count = lax.axis_size(ROW)
    chips = lax.axis_size(CHIP)
    is_first = position == 0
    is_last = position == count - 1
    is_odd = lax.axis_index("core") == 1
    on_last = lax.axis_index(CHIP) == chips - 1
    at = [lax.axis_index("y"), lax.axis_index("zh")]
    one = jnp.int32(1)
    held = jnp.where(is_first, 0, 1)
    index_a = jnp.stack([*at, one, held, one, held]).astype(jnp.int32)
    index_b = jnp.stack([*at, one, held]).astype(jnp.int32)
    ends = jnp.stack([is_first, is_last]).astype(jnp.int32)
    odd = is_odd.astype(jnp.int32).reshape(1)
    local, is_last, is_odd, on_last, index_a, index_b, ends, odd = lax.optimization_barrier(
        (local, is_last, is_odd, on_last, index_a, index_b, ends, odd)
    )
    n = eigenvectors.shape[0] // 2
    stay = jnp.stack([local[0, 1], local[1, 0], local[1, 1], local[2, 0]])
    half = 2 * stay.shape[1]
    before = ring(stay, "zh", 1)
    after = ring(stay, "zh", -1)
    from_next = shifted(local[0, 0], -1)
    from_prior = shifted(local[2, 1], 1)
    far = ring(before, "zh", 1)
    near_a = jnp.concatenate([stay, after, far, before], axis=1)
    before_a = ring(near_a, "y", 1)
    after_a = ring(near_a, "y", -1)
    give_a = (before_a[:, :half], after_a[:, half:])
    far0_a = ring(give_a[0], "y", 1)
    far1_a = ring(give_a[1], "y", -1)
    moved = jnp.stack([jnp.where(is_last, local[2, 1], from_next), from_prior])
    before = ring(moved, "y", 1)
    after = ring(moved, "y", -1)
    far = ring(moved, "y", 2)
    near_b = jnp.concatenate([moved, after, far, before], axis=1)
    before_b = ring(near_b, "zh", 1)
    after_b = ring(near_b, "zh", -1)
    give_b = after_these(before_b[:, :half], give_a), after_these(after_b[:, half:], give_a)
    far0_b = ring(give_b[0], "zh", 1)
    far1_b = ring(give_b[1], "zh", -1)
    mine = eigenvectors.T
    data = shifted(after_these(mine[:, :n], (near_b,)), -1)
    far0_a = after_these(far0_a, give_b)
    parts_a = prepare(True, index_a, near_a, after_a, before_a, far0_a, far1_a)
    parts_b = prepare(False, index_b, near_b, after_b, before_b, far0_b, far1_b)
    step, rest, add = operate(ends, data, mine, (*parts_a, *parts_b))

    swap = [(0, 1), (1, 0)]
    half = add.shape[0] // 2
    halves = add.reshape(2, half, 7 * n)
    keep = jnp.where(is_odd, halves[1], halves[0])
    give = jnp.where(is_odd, halves[0], halves[1])
    other = lax.ppermute(step, "core", swap)
    got = lax.ppermute(give, "core", swap)
    rest, other, got = lax.optimization_barrier((rest, other, got))
    high, low, chip_add = merge(odd, step, other, keep[:, : 3 * n], got[:, : 3 * n])
    other_rest = lax.ppermute(rest, "core", swap)

    sub = half // SUBS
    adds = [chip_add[k * sub : (k + 1) * sub] for k in range(SUBS)]
    arrived = [[lax.ppermute(part, CHIP, [(0, 1)])] for part in adds]
    for hop in range(2, chips):
        for k in range(SUBS):
            sent = hop_on(arrived[k][-1], high, low, adds[k])
            arrived[k].append(lax.ppermute(sent, CHIP, [(hop - 1, hop)]))
        if hop == 2:
            rest = after_these(rest, [sent])
            ended = ending(odd, step, other, rest, other_rest, keep, got)
        if hop == 3:
            *latest, high, low = lax.optimization_barrier((*[values[-1] for values in arrived], *ended, high, low))[:]
            for k in range(SUBS):
                arrived[k][-1] = latest[k]
            ended = latest[SUBS:]
    final = finish(arrived, *ended)
    for_prior, for_even, for_odd = [final[:, 2 * k * n : 2 * (k + 1) * n] for k in range(3)]
    got = lax.ppermute(jnp.where(is_odd, for_even, for_odd), "core", swap)
    handed = [
        lax.ppermute(for_prior, ROW, [(2 * (k + 1) + side, 2 * k + 1) for k in range(chips - 1)]) for side in range(2)
    ]
    got, *handed = lax.optimization_barrier((got, *handed))
    upper = jnp.where(is_odd, jnp.where(on_last, got, handed[0]), for_even)
    lower = jnp.where(is_odd, jnp.where(on_last, for_odd, handed[1]), got)
    return jnp.concatenate([upper, lower], axis=0).T


def solution(mesh):
    split_mesh = Mesh(mesh.devices.reshape(2, 4, 2, 4, 4), (*ROW, *COL))
    return jax.shard_map(
        shards,
        mesh=split_mesh,
        in_specs=(P(ROW, COL), P(None, ROW, None, COL)),
        out_specs=P(ROW, COL),
        check_vma=False,
    )
```

```python
import functools

import jax
import jax.numpy as jnp
from jax import lax
from jax.experimental import pallas as pl
from jax.experimental.pallas import tpu as pltpu
from jax.sharding import Mesh
from jax.sharding import PartitionSpec as P

ROW = ("zl", "x", "core")
CHIP = ("zl", "x")
COL = ("y", "zh")
SUBS = 2
INTERPRET = False

NN = (((1,), (0,)), ((), ()))
NT = (((1,), (1,)), ((), ()))


def split(value):
    high = value.astype(jnp.bfloat16)
    low = (value - high.astype(jnp.float32)).astype(jnp.bfloat16)
    return high, low


def dot3(left, right, dims=NN):
    (on_left,), (on_right,) = dims[0]
    long_left = jnp.concatenate([left[0], left[0], left[1]], axis=on_left)
    long_right = jnp.concatenate([right[0], right[1], right[0]], axis=on_right)
    return lax.dot_general(long_left, long_right, dims, preferred_element_type=jnp.float32)


def prepare_body(outer_y, index_ref, near_ref, after_ref, before_ref, far0_ref, far1_ref, high_ref, low_ref, v_ref, g_ref, p_ref):
    blocks, quarter, m = near_ref.shape
    n = 4 * quarter
    half = n // 2
    piece = quarter // 4
    at_y = index_ref[0]
    at_z = index_ref[1]
    for outer in range(4):
        for inner in range(4):
            dy, dz = (outer, inner) if outer_y else (inner, outer)
            start = lax.rem(at_y + dy, 4) * quarter + lax.rem(at_z + dz, 4) * piece
            at = pl.ds(inner * piece, piece)
            for block in range(blocks):
                if outer == 0:
                    part = near_ref[block, at, :]
                elif outer == 1:
                    part = after_ref[block, at, :]
                elif outer == 3:
                    part = before_ref[block, at, :]
                elif inner < 2:
                    part = far0_ref[block, at, :]
                else:
                    part = far1_ref[block, pl.ds((inner - 2) * piece, piece), :]
                v_ref[block, pl.ds(start, piece), :] = part
    rows = lax.broadcasted_iota(jnp.int32, (half, half), 0)
    cols = lax.broadcasted_iota(jnp.int32, (half, half), 1)
    eye = rows == cols
    pair = (rows // 2 == cols // 2) & (rows < cols)
    for block in range(blocks):
        vectors = split(v_ref[block])
        g_ref[block] = dot3(vectors, vectors, NT)
    problems = [(block, side) for block in range(blocks) for side in range(2)]
    for at, (block, side) in enumerate(problems):
        lo = side * half
        gram = g_ref[block, lo : lo + half, lo : lo + half]
        on_diagonal = jnp.where(eye, gram, 0.0)
        col_inverse = 1.0 / (0.5 * jnp.sum(on_diagonal, axis=1, keepdims=True))
        row_inverse = 1.0 / (0.5 * jnp.sum(on_diagonal, axis=0, keepdims=True))
        inverse = jnp.where(eye, col_inverse, 0.0)
        p_ref[at] = inverse - jnp.where(pair, gram * col_inverse * row_inverse, 0.0)

    levels = half.bit_length() - 1

    def level(power, carry):
        old_rows = jnp.right_shift(rows, power)
        old_cols = jnp.right_shift(cols, power)
        corner = (jnp.right_shift(old_rows, 1) == jnp.right_shift(old_cols, 1)) & (old_rows < old_cols)
        first = []
        for at, (block, side) in enumerate(problems):
            lo = side * half
            edge = split(jnp.where(corner, g_ref[block, lo : lo + half, lo : lo + half], 0.0))
            first.append(dot3(split(p_ref[at]), edge))
        for at in range(len(problems)):
            old = p_ref[at]
            p_ref[at] = old - dot3(split(first[at]), split(old))
        return carry

    lax.fori_loop(1, levels, level, 0)
    eye = lax.broadcasted_iota(jnp.int32, (m, m), 0) == lax.broadcasted_iota(jnp.int32, (m, m), 1)
    unit = jnp.where(eye, 1.0, 0.0)
    first = [
        dot3(split(p_ref[2 * block]), split(g_ref[block, :half, half:])) for block in range(blocks)
    ]
    corners = [dot3(split(first[block]), split(p_ref[2 * block + 1])) for block in range(blocks)]
    for block in range(blocks):
        vectors = split(v_ref[block])
        top = split(jnp.concatenate([p_ref[2 * block], -corners[block]], axis=1))
        low = split(p_ref[2 * block + 1])
        upper = dot3(top, vectors)
        lower = dot3(low, (vectors[0][half:], vectors[1][half:]))
        scaled = split(jnp.concatenate([upper, lower], axis=0).T)
        whole = unit - dot3(scaled, vectors)
        whole = jnp.where(index_ref[2 + block] == 1, whole, unit)
        high, low = split(whole)
        high_ref[block] = high
        low_ref[block] = low


def prepare(outer_y, index, near, after, before, far0, far1):
    blocks, quarter, m = near.shape
    n = 4 * quarter
    out = jax.ShapeDtypeStruct((blocks, m, m), jnp.bfloat16)
    vmem = pl.BlockSpec(memory_space=pltpu.VMEM)
    return pl.pallas_call(
        functools.partial(prepare_body, outer_y),
        out_shape=(out, out),
        in_specs=[pl.BlockSpec(memory_space=pltpu.SMEM)] + [vmem] * 5,
        out_specs=(vmem, vmem),
        scratch_shapes=[
            pltpu.VMEM((blocks, n, m), jnp.float32),
            pltpu.VMEM((blocks, n, n), jnp.float32),
            pltpu.VMEM((2 * blocks, n // 2, n // 2), jnp.float32),
        ],
        compiler_params=pltpu.CompilerParams(vmem_limit_bytes=14 * 1024 * 1024),
        cost_estimate=pl.CostEstimate(flops=2_000_000_000, bytes_accessed=1_000_000, transcendentals=0),
        interpret=INTERPRET,
        name="prepare",
    )(index, near, after, before, far0, far1)


PAIRS = ((0, 0), (0, 1), (0, 2), (1, 1), (1, 2), (2, 2))


def operate_body(ends_ref, data_ref, own_ref, ah, al, bh, bl, step_ref, rest_ref, add_ref):
    n = ah.shape[1] // 2
    first = ends_ref[0] == 1
    last = ends_ref[1] == 1
    width = data_ref.shape[1]
    held = {(0, 0): (ah, al, 0), (0, 1): (bh, bl, 0), (1, 0): (ah, al, 1), (1, 1): (ah, al, 2), (2, 0): (bh, bl, 1), (2, 1): (ah, al, 3)}

    def part(sweep, block, side=None):
        high, low, at = held[sweep, block]
        if side is None:
            return high[at], low[at]
        rows = pl.ds(side * n, n)
        return high[at, rows, :], low[at, rows, :]

    for sweep in range(3):
        a_top = part(sweep, 0, 0)
        b_top = part(sweep, 1, 0)
        b_low = part(sweep, 1, 1)
        fresh = a_top[0].astype(jnp.float32) + a_top[1].astype(jnp.float32)
        if sweep == 0:
            own = own_ref[...].T
            arriving = jnp.where(first, own[:, :n], 0.0)
            mid = dot3(split(jnp.concatenate([arriving, own[:, n:]], axis=1)), part(0, 0))
            mid = jnp.concatenate([fresh, mid], axis=0)
            v = data_ref[...].T
            done = dot3(split(mid[:, n:]), b_top)
            done = jnp.concatenate([done[:n], done[n:] + dot3(split(v), b_low)], axis=0)
            v = jnp.concatenate([jnp.zeros((n, n), jnp.float32), v], axis=0)
            done = jnp.where(last, jnp.concatenate([mid[:, n:], v], axis=1), done)
        else:
            mid = dot3(split(u), part(sweep, 0, 1))
            mid = jnp.concatenate([mid[:-width], fresh, mid[-width:]], axis=0)
            done = dot3(split(mid[:, n:]), b_top)
            more = dot3(split(v), b_low)
            early = sweep * n
            done = jnp.concatenate(
                [done[:early] + more[:early], done[early : early + n], done[early + n :] + more[early:]], axis=0
            )
        known = (sweep + 1) * n
        u, v = mid[:, :n], done[:, :n]
        out = done[:, n:]
        for k in range(sweep + 1):
            step_ref[PAIRS.index((k, sweep))] = out[k * n : (k + 1) * n]
        add_ref[:, sweep * n : (sweep + 1) * n] = out[known:]
    rest_ref[:, 0:n] = u[: 3 * n]
    rest_ref[:, n : 2 * n] = v[: 3 * n]
    add_ref[:, 3 * n : 4 * n] = u[3 * n :]
    add_ref[:, 4 * n : 5 * n] = v[3 * n :]

    @pl.when(last)
    def _():
        high, low = bh[0], bl[0]
        for k in range(4):
            if k < 3:
                upper = step_ref[PAIRS.index((k, 2))]
                lower = step_ref[PAIRS.index((k, 1))] if k < 2 else jnp.zeros((n, n), jnp.float32)
            else:
                upper = add_ref[:, 2 * n : 3 * n]
                lower = add_ref[:, n : 2 * n]
            result = dot3(split(jnp.concatenate([upper, lower], axis=1)), (high, low))
            if k < 3:
                rest_ref[k * n : (k + 1) * n, 2 * n :] = result
            else:
                add_ref[:, 5 * n :] = result

    @pl.when(jnp.logical_not(last))
    def _():
        rest_ref[:, 2 * n :] = jnp.zeros((3 * n, 2 * n), jnp.float32)
        add_ref[:, 5 * n :] = jnp.zeros((width, 2 * n), jnp.float32)


def operate(ends, data, own, parts):
    m, width = own.shape
    n = m // 2
    vmem = pl.BlockSpec(memory_space=pltpu.VMEM)
    return pl.pallas_call(
        operate_body,
        out_shape=(
            jax.ShapeDtypeStruct((6, n, n), jnp.float32),
            jax.ShapeDtypeStruct((3 * n, 4 * n), jnp.float32),
            jax.ShapeDtypeStruct((width, 7 * n), jnp.float32),
        ),
        in_specs=[pl.BlockSpec(memory_space=pltpu.SMEM)] + [vmem] * 6,
        out_specs=(vmem,) * 3,
        compiler_params=pltpu.CompilerParams(vmem_limit_bytes=20 * 1024 * 1024),
        interpret=INTERPRET,
        name="operate",
    )(ends, data, own, *parts)


def merge_body(odd_ref, mine_ref, other_ref, keep_ref, got_ref, high_ref, low_ref, add_ref):
    n = mine_ref.shape[1]
    odd = odd_ref[0] == 1
    keep = keep_ref[...]
    got = got_ref[...]
    even_parts = [split(jnp.where(odd, other_ref[k], mine_ref[k])) for k in range(6)]
    odd_parts = [split(jnp.where(odd, mine_ref[k], other_ref[k])) for k in range(6)]
    odd_add = jnp.where(odd, keep, got)
    add_parts = split(jnp.where(odd, got, keep))
    for s in range(3):
        total = odd_add[:, s * n : (s + 1) * n]
        for j in range(s + 1):
            columns = slice(j * n, (j + 1) * n)
            total = total + dot3((add_parts[0][:, columns], add_parts[1][:, columns]), odd_parts[PAIRS.index((j, s))])
        add_ref[:, s * n : (s + 1) * n] = total
        for k in range(s + 1):
            total = None
            for j in range(k, s + 1):
                term = dot3(even_parts[PAIRS.index((k, j))], odd_parts[PAIRS.index((j, s))])
                total = term if total is None else total + term
            high_ref[PAIRS.index((k, s))], low_ref[PAIRS.index((k, s))] = split(total)


def merge(odd, mine, other, keep, got):
    n = mine.shape[1]
    half = keep.shape[0]
    vmem = pl.BlockSpec(memory_space=pltpu.VMEM)
    packed = jax.ShapeDtypeStruct((6, n, n), jnp.bfloat16)
    return pl.pallas_call(
        merge_body,
        out_shape=(packed, packed, jax.ShapeDtypeStruct((half, 3 * n), jnp.float32)),
        in_specs=[pl.BlockSpec(memory_space=pltpu.SMEM)] + [vmem] * 4,
        out_specs=(vmem,) * 3,
        compiler_params=pltpu.CompilerParams(vmem_limit_bytes=20 * 1024 * 1024),
        interpret=INTERPRET,
        name="merge",
    )(odd, mine, other, keep, got)


def hop_body(state_ref, high_ref, low_ref, add_ref, out_ref):
    n = high_ref.shape[1]
    high, low = split(state_ref[...])
    count = high.shape[0]
    both = jnp.concatenate([high, low], axis=0)
    for s in range(3):
        total = add_ref[:, s * n : (s + 1) * n]
        for k in range(s + 1):
            at = PAIRS.index((k, s))
            columns = slice(k * n, (k + 1) * n)
            main = lax.dot_general(both[:, columns], high_ref[at], NN, preferred_element_type=jnp.float32)
            side = lax.dot_general(high[:, columns], low_ref[at], NN, preferred_element_type=jnp.float32)
            total = total + (main[:count] + (main[count:] + side))
        out_ref[:, s * n : (s + 1) * n] = total


def hop_on(state, high, low, add):
    vmem = pl.BlockSpec(memory_space=pltpu.VMEM)
    return pl.pallas_call(
        hop_body,
        out_shape=jax.ShapeDtypeStruct(state.shape, jnp.float32),
        in_specs=[vmem] * 4,
        out_specs=vmem,
        compiler_params=pltpu.CompilerParams(vmem_limit_bytes=8 * 1024 * 1024),
        interpret=INTERPRET,
        name="hop",
    )(state, high, low, add)


def ending_body(odd_ref, mine_ref, other_ref, rest_ref, other_rest_ref, keep_ref, got_ref, high_ref, low_ref, add_ref):
    n = mine_ref.shape[1]
    odd = odd_ref[0] == 1
    for k in range(3):
        rows = slice(k * n, (k + 1) * n)
        even_rest = jnp.where(odd, other_rest_ref[rows, : 2 * n], rest_ref[rows, : 2 * n])
        high_ref[rows, : 2 * n], low_ref[rows, : 2 * n] = split(even_rest)
    odd_parts = []
    for k in range(3):
        rows = slice(k * n, (k + 1) * n)
        odd_parts.append(split(jnp.where(odd, rest_ref[rows, :], other_rest_ref[rows, :])))
    for k in range(3):
        total = None
        for j in range(k, 3):
            at = PAIRS.index((k, j))
            term = dot3(split(jnp.where(odd, other_ref[at], mine_ref[at])), odd_parts[j])
            total = term if total is None else total + term
        rows = slice(k * n, (k + 1) * n)
        high_ref[rows, 2 * n :], low_ref[rows, 2 * n :] = split(total)
    even_add = jnp.where(odd, got_ref[...], keep_ref[...])
    odd_add = jnp.where(odd, keep_ref[...], got_ref[...])
    total = odd_add[:, 3 * n :]
    for j in range(3):
        total = total + dot3(split(even_add[:, j * n : (j + 1) * n]), odd_parts[j])
    add_ref[:, : 2 * n] = even_add[:, 3 * n : 5 * n]
    add_ref[:, 2 * n :] = total


def ending(odd, mine, other, rest, other_rest, keep, got):
    n = mine.shape[1]
    vmem = pl.BlockSpec(memory_space=pltpu.VMEM)
    wide = jax.ShapeDtypeStruct((3 * n, 6 * n), jnp.bfloat16)
    return pl.pallas_call(
        ending_body,
        out_shape=(wide, wide, jax.ShapeDtypeStruct((keep.shape[0], 6 * n), jnp.float32)),
        in_specs=[pl.BlockSpec(memory_space=pltpu.SMEM)] + [vmem] * 6,
        out_specs=(vmem,) * 3,
        compiler_params=pltpu.CompilerParams(vmem_limit_bytes=16 * 1024 * 1024),
        interpret=INTERPRET,
        name="ending",
    )(odd, mine, other, rest, other_rest, keep, got)


def finish_body(*refs):
    *state_refs, high_ref, low_ref, add_ref, out_ref = refs
    hops = len(state_refs) // SUBS
    rows = []
    for k in range(SUBS):
        total = state_refs[k * hops][...]
        for ref in state_refs[k * hops + 1 : (k + 1) * hops]:
            total = total + ref[...]
        rows.append(total)
    state = split(jnp.concatenate(rows, axis=0))
    out_ref[...] = dot3(state, (high_ref[...], low_ref[...])) + add_ref[...]


def finish(arrived, high, low, add):
    vmem = pl.BlockSpec(memory_space=pltpu.VMEM)
    states = [value for values in arrived for value in values]
    return pl.pallas_call(
        finish_body,
        out_shape=jax.ShapeDtypeStruct(add.shape, jnp.float32),
        in_specs=[vmem] * (len(states) + 3),
        out_specs=vmem,
        compiler_params=pltpu.CompilerParams(vmem_limit_bytes=16 * 1024 * 1024),
        interpret=INTERPRET,
        name="finish",
    )(*states, high, low, add)


def ring(value, axis, step):
    count = lax.axis_size(axis)
    return lax.ppermute(value, axis, [(k, (k + step) % count) for k in range(count)])


def shifted(value, step):
    count = lax.axis_size(ROW)
    return lax.ppermute(value, ROW, [(k, k + step) for k in range(max(0, -step), min(count, count - step))])


def after_these(value, others):
    return lax.optimization_barrier((value, *others))[0]


def shards(eigenvectors, householder):
    local = jnp.swapaxes(householder, 2, 3)
    position = lax.axis_index(ROW)
    count = lax.axis_size(ROW)
    chips = lax.axis_size(CHIP)
    is_first = position == 0
    is_last = position == count - 1
    is_odd = lax.axis_index("core") == 1
    flipped = lax.axis_index(CHIP) % 2 == 1
    takes_second = is_odd != flipped
    on_last = lax.axis_index(CHIP) == chips - 1
    at = [lax.axis_index("y"), lax.axis_index("zh")]
    one = jnp.int32(1)
    held = jnp.where(is_first, 0, 1)
    index_a = jnp.stack([*at, one, held, one, held]).astype(jnp.int32)
    index_b = jnp.stack([*at, one, held]).astype(jnp.int32)
    ends = jnp.stack([is_first, is_last]).astype(jnp.int32)
    odd = is_odd.astype(jnp.int32).reshape(1)
    local, is_last, is_odd, flipped, takes_second, on_last, index_a, index_b, ends, odd = lax.optimization_barrier(
        (local, is_last, is_odd, flipped, takes_second, on_last, index_a, index_b, ends, odd)
    )
    n = eigenvectors.shape[0] // 2
    stay = jnp.stack([local[0, 1], local[1, 0], local[1, 1], local[2, 0]])
    half = 2 * stay.shape[1]
    before = ring(stay, "zh", 1)
    after = ring(stay, "zh", -1)
    from_next = shifted(local[0, 0], -1)
    from_prior = shifted(local[2, 1], 1)
    far = ring(before, "zh", 1)
    near_a = jnp.concatenate([stay, after, far, before], axis=1)
    moved = jnp.stack([jnp.where(is_last, local[2, 1], from_next), from_prior])
    before = ring(moved, "y", 1)
    after = ring(moved, "y", -1)
    far = ring(moved, "y", 2)
    near_b = jnp.concatenate([moved, after, far, before], axis=1)
    near_a = after_these(near_a, (before, after, far))
    before_a = ring(near_a, "y", 1)
    after_a = ring(near_a, "y", -1)
    give_a = (before_a[:, :half], after_a[:, half:])
    far0_a = ring(give_a[0], "y", 1)
    far1_a = ring(give_a[1], "y", -1)
    before_b = ring(near_b, "zh", 1)
    after_b = ring(near_b, "zh", -1)
    give_b0 = before_b[:, :half]
    give_b1 = after_b[:, half:]
    give_b = after_these(give_b0, give_a), after_these(give_b1, give_a)
    far0_b = ring(give_b[0], "zh", 1)
    far1_b = ring(give_b[1], "zh", -1)
    data = shifted(after_these(eigenvectors[:n], (near_b,)), -1)
    far0_a = after_these(far0_a, give_b)
    parts_a = prepare(True, index_a, near_a, after_a, before_a, far0_a, far1_a)
    parts_b = prepare(False, index_b, after_these(near_b, parts_a), after_b, before_b, far0_b, far1_b)
    step, rest, add = operate(ends, data, eigenvectors, (*parts_a, *parts_b))

    swap = [(0, 1), (1, 0)]
    half = add.shape[0] // 2
    halves = add.reshape(2, half, 7 * n)
    keep = jnp.where(takes_second, halves[1], halves[0])
    give = jnp.where(takes_second, halves[0], halves[1])
    other = lax.ppermute(step, "core", swap)
    got = lax.ppermute(give, "core", swap)
    rest, other, got = lax.optimization_barrier((rest, other, got))
    high, low, chip_add = merge(odd, step, other, keep[:, : 3 * n], got[:, : 3 * n])
    other_rest = lax.ppermute(rest, "core", swap)

    sub = half // SUBS
    adds = [chip_add[k * sub : (k + 1) * sub] for k in range(SUBS)]

    def onward(value, hop):
        return lax.ppermute(value, ROW, [(2 * hop - 2 + side, 2 * hop + 1 - side) for side in range(2)])

    arrived = [[onward(part, 1)] for part in adds]
    for hop in range(2, chips):
        for k in range(SUBS):
            sent = hop_on(arrived[k][-1], high, low, adds[k])
            arrived[k].append(onward(sent, hop))
        if hop == 2:
            rest = after_these(rest, [sent])
            ended = ending(odd, step, other, rest, other_rest, keep, got)
        if hop == 3:
            *latest, high, low = lax.optimization_barrier((*[values[-1] for values in arrived], *ended, high, low))[:]
            for k in range(SUBS):
                arrived[k][-1] = latest[k]
            ended = latest[SUBS:]
    final = finish(arrived, *ended)
    for_prior, for_even, for_odd = [final[:, 2 * k * n : 2 * (k + 1) * n] for k in range(3)]
    got = lax.ppermute(jnp.where(is_odd, for_even, for_odd), "core", swap)
    handed = [
        lax.ppermute(for_prior, ROW, [(2 * (k + 1) + side, 2 * k + 1) for k in range(chips - 1)]) for side in range(2)
    ]
    got, *handed = lax.optimization_barrier((got, *handed))
    one_half = jnp.where(is_odd, jnp.where(on_last, got, handed[1]), for_even)
    other_half = jnp.where(is_odd, jnp.where(on_last, for_odd, handed[0]), got)
    upper = jnp.where(flipped, other_half, one_half)
    lower = jnp.where(flipped, one_half, other_half)
    return jnp.concatenate([upper, lower], axis=0).T


def solution(mesh):
    split_mesh = Mesh(mesh.devices.reshape(2, 4, 2, 4, 4), (*ROW, *COL))
    return jax.shard_map(
        shards,
        mesh=split_mesh,
        in_specs=(P(ROW, COL), P(None, ROW, None, COL)),
        out_specs=P(ROW, COL),
        check_vma=False,
    )
```

```python
import functools

import jax
import jax.numpy as jnp
from jax import lax
from jax.experimental import pallas as pl
from jax.experimental.pallas import tpu as pltpu
from jax.sharding import Mesh
from jax.sharding import PartitionSpec as P

ROW = ("zl", "x", "core")
CHIP = ("zl", "x")
COL = ("y", "zh")
SUBS = 2
INTERPRET = False

NN = (((1,), (0,)), ((), ()))
NT = (((1,), (1,)), ((), ()))


def split(value):
    high = value.astype(jnp.bfloat16)
    low = (value - high.astype(jnp.float32)).astype(jnp.bfloat16)
    return high, low


def dot3(left, right, dims=NN):
    (on_left,), (on_right,) = dims[0]
    long_left = jnp.concatenate([left[0], left[0], left[1]], axis=on_left)
    long_right = jnp.concatenate([right[0], right[1], right[0]], axis=on_right)
    return lax.dot_general(long_left, long_right, dims, preferred_element_type=jnp.float32)


def prepare_body(outer_y, index_ref, near_ref, after_ref, before_ref, far0_ref, far1_ref, high_ref, low_ref, v_ref, g_ref, p_ref):
    blocks, quarter, m = near_ref.shape
    n = 4 * quarter
    half = n // 2
    piece = quarter // 4
    at_y = index_ref[0]
    at_z = index_ref[1]
    for outer in range(4):
        for inner in range(4):
            dy, dz = (outer, inner) if outer_y else (inner, outer)
            start = lax.rem(at_y + dy, 4) * quarter + lax.rem(at_z + dz, 4) * piece
            at = pl.ds(inner * piece, piece)
            for block in range(blocks):
                if outer == 0:
                    part = near_ref[block, at, :]
                elif outer == 1:
                    part = after_ref[block, at, :]
                elif outer == 3:
                    part = before_ref[block, at, :]
                elif inner < 2:
                    part = far0_ref[block, at, :]
                else:
                    part = far1_ref[block, pl.ds((inner - 2) * piece, piece), :]
                v_ref[block, pl.ds(start, piece), :] = part
    rows = lax.broadcasted_iota(jnp.int32, (half, half), 0)
    cols = lax.broadcasted_iota(jnp.int32, (half, half), 1)
    eye = rows == cols
    pair = (rows // 2 == cols // 2) & (rows < cols)
    for block in range(blocks):
        vectors = split(v_ref[block])
        g_ref[block] = dot3(vectors, vectors, NT)
    problems = [(block, side) for block in range(blocks) for side in range(2)]
    for at, (block, side) in enumerate(problems):
        lo = side * half
        gram = g_ref[block, lo : lo + half, lo : lo + half]
        on_diagonal = jnp.where(eye, gram, 0.0)
        col_inverse = 1.0 / (0.5 * jnp.sum(on_diagonal, axis=1, keepdims=True))
        row_inverse = 1.0 / (0.5 * jnp.sum(on_diagonal, axis=0, keepdims=True))
        inverse = jnp.where(eye, col_inverse, 0.0)
        p_ref[at] = inverse - jnp.where(pair, gram * col_inverse * row_inverse, 0.0)

    levels = half.bit_length() - 1

    def level(power, carry):
        old_rows = jnp.right_shift(rows, power)
        old_cols = jnp.right_shift(cols, power)
        corner = (jnp.right_shift(old_rows, 1) == jnp.right_shift(old_cols, 1)) & (old_rows < old_cols)
        first = []
        for at, (block, side) in enumerate(problems):
            lo = side * half
            edge = split(jnp.where(corner, g_ref[block, lo : lo + half, lo : lo + half], 0.0))
            first.append(dot3(split(p_ref[at]), edge))
        for at in range(len(problems)):
            old = p_ref[at]
            p_ref[at] = old - dot3(split(first[at]), split(old))
        return carry

    lax.fori_loop(1, levels, level, 0)
    eye = lax.broadcasted_iota(jnp.int32, (m, m), 0) == lax.broadcasted_iota(jnp.int32, (m, m), 1)
    unit = jnp.where(eye, 1.0, 0.0)
    first = [
        dot3(split(p_ref[2 * block]), split(g_ref[block, :half, half:])) for block in range(blocks)
    ]
    corners = [dot3(split(first[block]), split(p_ref[2 * block + 1])) for block in range(blocks)]
    for block in range(blocks):
        vectors = split(v_ref[block])
        top = split(jnp.concatenate([p_ref[2 * block], -corners[block]], axis=1))
        low = split(p_ref[2 * block + 1])
        upper = dot3(top, vectors)
        lower = dot3(low, (vectors[0][half:], vectors[1][half:]))
        scaled = split(jnp.concatenate([upper, lower], axis=0).T)
        whole = unit - dot3(scaled, vectors)
        whole = jnp.where(index_ref[2 + block] == 1, whole, unit)
        high, low = split(whole)
        high_ref[block] = high
        low_ref[block] = low


def prepare(outer_y, index, near, after, before, far0, far1):
    blocks, quarter, m = near.shape
    n = 4 * quarter
    out = jax.ShapeDtypeStruct((blocks, m, m), jnp.bfloat16)
    vmem = pl.BlockSpec(memory_space=pltpu.VMEM)
    return pl.pallas_call(
        functools.partial(prepare_body, outer_y),
        out_shape=(out, out),
        in_specs=[pl.BlockSpec(memory_space=pltpu.SMEM)] + [vmem] * 5,
        out_specs=(vmem, vmem),
        scratch_shapes=[
            pltpu.VMEM((blocks, n, m), jnp.float32),
            pltpu.VMEM((blocks, n, n), jnp.float32),
            pltpu.VMEM((2 * blocks, n // 2, n // 2), jnp.float32),
        ],
        compiler_params=pltpu.CompilerParams(vmem_limit_bytes=14 * 1024 * 1024),
        cost_estimate=pl.CostEstimate(flops=2_000_000_000, bytes_accessed=1_000_000, transcendentals=0),
        interpret=INTERPRET,
        name="prepare",
    )(index, near, after, before, far0, far1)


PAIRS = ((0, 0), (0, 1), (0, 2), (1, 1), (1, 2), (2, 2))


def operate_body(ends_ref, data_ref, own_ref, ah, al, bh, bl, step_ref, rest_ref, add_ref):
    n = ah.shape[1] // 2
    first = ends_ref[0] == 1
    last = ends_ref[1] == 1
    width = data_ref.shape[1]
    held = {(0, 0): (ah, al, 0), (0, 1): (bh, bl, 0), (1, 0): (ah, al, 1), (1, 1): (ah, al, 2), (2, 0): (bh, bl, 1), (2, 1): (ah, al, 3)}

    def part(sweep, block, side=None):
        high, low, at = held[sweep, block]
        if side is None:
            return high[at], low[at]
        rows = pl.ds(side * n, n)
        return high[at, rows, :], low[at, rows, :]

    for sweep in range(3):
        a_top = part(sweep, 0, 0)
        b_top = part(sweep, 1, 0)
        b_low = part(sweep, 1, 1)
        fresh = a_top[0].astype(jnp.float32) + a_top[1].astype(jnp.float32)
        if sweep == 0:
            own = own_ref[...].T
            arriving = jnp.where(first, own[:, :n], 0.0)
            mid = dot3(split(jnp.concatenate([arriving, own[:, n:]], axis=1)), part(0, 0))
            mid = jnp.concatenate([fresh, mid], axis=0)
            v = data_ref[...].T
            done = dot3(split(mid[:, n:]), b_top)
            done = jnp.concatenate([done[:n], done[n:] + dot3(split(v), b_low)], axis=0)
            v = jnp.concatenate([jnp.zeros((n, n), jnp.float32), v], axis=0)
            done = jnp.where(last, jnp.concatenate([mid[:, n:], v], axis=1), done)
        else:
            mid = dot3(split(u), part(sweep, 0, 1))
            mid = jnp.concatenate([mid[:-width], fresh, mid[-width:]], axis=0)
            done = dot3(split(mid[:, n:]), b_top)
            more = dot3(split(v), b_low)
            early = sweep * n
            done = jnp.concatenate(
                [done[:early] + more[:early], done[early : early + n], done[early + n :] + more[early:]], axis=0
            )
        known = (sweep + 1) * n
        u, v = mid[:, :n], done[:, :n]
        out = done[:, n:]
        for k in range(sweep + 1):
            step_ref[PAIRS.index((k, sweep))] = out[k * n : (k + 1) * n]
        add_ref[:, sweep * n : (sweep + 1) * n] = out[known:]
    rest_ref[:, 0:n] = u[: 3 * n]
    rest_ref[:, n : 2 * n] = v[: 3 * n]
    add_ref[:, 3 * n : 4 * n] = u[3 * n :]
    add_ref[:, 4 * n : 5 * n] = v[3 * n :]

    @pl.when(last)
    def _():
        high, low = bh[0], bl[0]
        for k in range(4):
            if k < 3:
                upper = step_ref[PAIRS.index((k, 2))]
                lower = step_ref[PAIRS.index((k, 1))] if k < 2 else jnp.zeros((n, n), jnp.float32)
            else:
                upper = add_ref[:, 2 * n : 3 * n]
                lower = add_ref[:, n : 2 * n]
            result = dot3(split(jnp.concatenate([upper, lower], axis=1)), (high, low))
            if k < 3:
                rest_ref[k * n : (k + 1) * n, 2 * n :] = result
            else:
                add_ref[:, 5 * n :] = result

    @pl.when(jnp.logical_not(last))
    def _():
        rest_ref[:, 2 * n :] = jnp.zeros((3 * n, 2 * n), jnp.float32)
        add_ref[:, 5 * n :] = jnp.zeros((width, 2 * n), jnp.float32)


def operate(ends, data, own, parts):
    m, width = own.shape
    n = m // 2
    vmem = pl.BlockSpec(memory_space=pltpu.VMEM)
    return pl.pallas_call(
        operate_body,
        out_shape=(
            jax.ShapeDtypeStruct((6, n, n), jnp.float32),
            jax.ShapeDtypeStruct((3 * n, 4 * n), jnp.float32),
            jax.ShapeDtypeStruct((width, 7 * n), jnp.float32),
        ),
        in_specs=[pl.BlockSpec(memory_space=pltpu.SMEM)] + [vmem] * 6,
        out_specs=(vmem,) * 3,
        compiler_params=pltpu.CompilerParams(vmem_limit_bytes=20 * 1024 * 1024),
        interpret=INTERPRET,
        name="operate",
    )(ends, data, own, *parts)


def merge_body(odd_ref, mine_ref, other_ref, keep_ref, got_ref, high_ref, low_ref, add_ref):
    n = mine_ref.shape[1]
    odd = odd_ref[0] == 1
    keep = keep_ref[...]
    got = got_ref[...]
    even_parts = [split(jnp.where(odd, other_ref[k], mine_ref[k])) for k in range(6)]
    odd_parts = [split(jnp.where(odd, mine_ref[k], other_ref[k])) for k in range(6)]
    odd_add = jnp.where(odd, keep, got)
    add_parts = split(jnp.where(odd, got, keep))
    for s in range(3):
        total = odd_add[:, s * n : (s + 1) * n]
        for j in range(s + 1):
            columns = slice(j * n, (j + 1) * n)
            total = total + dot3((add_parts[0][:, columns], add_parts[1][:, columns]), odd_parts[PAIRS.index((j, s))])
        add_ref[:, s * n : (s + 1) * n] = total
        for k in range(s + 1):
            total = None
            for j in range(k, s + 1):
                term = dot3(even_parts[PAIRS.index((k, j))], odd_parts[PAIRS.index((j, s))])
                total = term if total is None else total + term
            high_ref[PAIRS.index((k, s))], low_ref[PAIRS.index((k, s))] = split(total)


def merge(odd, mine, other, keep, got):
    n = mine.shape[1]
    half = keep.shape[0]
    vmem = pl.BlockSpec(memory_space=pltpu.VMEM)
    packed = jax.ShapeDtypeStruct((6, n, n), jnp.bfloat16)
    return pl.pallas_call(
        merge_body,
        out_shape=(packed, packed, jax.ShapeDtypeStruct((half, 3 * n), jnp.float32)),
        in_specs=[pl.BlockSpec(memory_space=pltpu.SMEM)] + [vmem] * 4,
        out_specs=(vmem,) * 3,
        compiler_params=pltpu.CompilerParams(vmem_limit_bytes=20 * 1024 * 1024),
        interpret=INTERPRET,
        name="merge",
    )(odd, mine, other, keep, got)


def hop_body(state_ref, high_ref, low_ref, add_ref, out_ref):
    n = high_ref.shape[1]
    high, low = split(state_ref[...])
    count = high.shape[0]
    both = jnp.concatenate([high, low], axis=0)
    for s in range(3):
        total = add_ref[:, s * n : (s + 1) * n]
        for k in range(s + 1):
            at = PAIRS.index((k, s))
            columns = slice(k * n, (k + 1) * n)
            main = lax.dot_general(both[:, columns], high_ref[at], NN, preferred_element_type=jnp.float32)
            side = lax.dot_general(high[:, columns], low_ref[at], NN, preferred_element_type=jnp.float32)
            total = total + (main[:count] + (main[count:] + side))
        out_ref[:, s * n : (s + 1) * n] = total


def hop_on(state, high, low, add):
    vmem = pl.BlockSpec(memory_space=pltpu.VMEM)
    return pl.pallas_call(
        hop_body,
        out_shape=jax.ShapeDtypeStruct(state.shape, jnp.float32),
        in_specs=[vmem] * 4,
        out_specs=vmem,
        compiler_params=pltpu.CompilerParams(vmem_limit_bytes=8 * 1024 * 1024),
        interpret=INTERPRET,
        name="hop",
    )(state, high, low, add)


def ending_body(odd_ref, mine_ref, other_ref, rest_ref, other_rest_ref, keep_ref, got_ref, high_ref, low_ref, add_ref):
    n = mine_ref.shape[1]
    odd = odd_ref[0] == 1
    for k in range(3):
        rows = slice(k * n, (k + 1) * n)
        even_rest = jnp.where(odd, other_rest_ref[rows, : 2 * n], rest_ref[rows, : 2 * n])
        high_ref[rows, : 2 * n], low_ref[rows, : 2 * n] = split(even_rest)
    odd_parts = []
    for k in range(3):
        rows = slice(k * n, (k + 1) * n)
        odd_parts.append(split(jnp.where(odd, rest_ref[rows, :], other_rest_ref[rows, :])))
    for k in range(3):
        total = None
        for j in range(k, 3):
            at = PAIRS.index((k, j))
            term = dot3(split(jnp.where(odd, other_ref[at], mine_ref[at])), odd_parts[j])
            total = term if total is None else total + term
        rows = slice(k * n, (k + 1) * n)
        high_ref[rows, 2 * n :], low_ref[rows, 2 * n :] = split(total)
    even_add = jnp.where(odd, got_ref[...], keep_ref[...])
    odd_add = jnp.where(odd, keep_ref[...], got_ref[...])
    total = odd_add[:, 3 * n :]
    for j in range(3):
        total = total + dot3(split(even_add[:, j * n : (j + 1) * n]), odd_parts[j])
    add_ref[:, : 2 * n] = even_add[:, 3 * n : 5 * n]
    add_ref[:, 2 * n :] = total


def ending(odd, mine, other, rest, other_rest, keep, got):
    n = mine.shape[1]
    vmem = pl.BlockSpec(memory_space=pltpu.VMEM)
    wide = jax.ShapeDtypeStruct((3 * n, 6 * n), jnp.bfloat16)
    return pl.pallas_call(
        ending_body,
        out_shape=(wide, wide, jax.ShapeDtypeStruct((keep.shape[0], 6 * n), jnp.float32)),
        in_specs=[pl.BlockSpec(memory_space=pltpu.SMEM)] + [vmem] * 6,
        out_specs=(vmem,) * 3,
        compiler_params=pltpu.CompilerParams(vmem_limit_bytes=16 * 1024 * 1024),
        interpret=INTERPRET,
        name="ending",
    )(odd, mine, other, rest, other_rest, keep, got)


def finish_body(*refs):
    *state_refs, high_ref, low_ref, add_ref, out_ref = refs
    hops = len(state_refs) // SUBS
    rows = []
    for k in range(SUBS):
        total = state_refs[k * hops][...]
        for ref in state_refs[k * hops + 1 : (k + 1) * hops]:
            total = total + ref[...]
        rows.append(total)
    state = split(jnp.concatenate(rows, axis=0))
    out_ref[...] = dot3(state, (high_ref[...], low_ref[...])) + add_ref[...]


def finish(arrived, high, low, add):
    vmem = pl.BlockSpec(memory_space=pltpu.VMEM)
    states = [value for values in arrived for value in values]
    return pl.pallas_call(
        finish_body,
        out_shape=jax.ShapeDtypeStruct(add.shape, jnp.float32),
        in_specs=[vmem] * (len(states) + 3),
        out_specs=vmem,
        compiler_params=pltpu.CompilerParams(vmem_limit_bytes=16 * 1024 * 1024),
        interpret=INTERPRET,
        name="finish",
    )(*states, high, low, add)


def ring(value, axis, step):
    count = lax.axis_size(axis)
    return lax.ppermute(value, axis, [(k, (k + step) % count) for k in range(count)])


def shifted(value, step):
    count = lax.axis_size(ROW)
    return lax.ppermute(value, ROW, [(k, k + step) for k in range(max(0, -step), min(count, count - step))])


def after_these(value, others):
    return lax.optimization_barrier((value, *others))[0]


def shards(eigenvectors, householder):
    local = jnp.swapaxes(householder, 2, 3)
    position = lax.axis_index(ROW)
    count = lax.axis_size(ROW)
    chips = lax.axis_size(CHIP)
    is_first = position == 0
    is_last = position == count - 1
    is_odd = lax.axis_index("core") == 1
    on_last = lax.axis_index(CHIP) == chips - 1
    at = [lax.axis_index("y"), lax.axis_index("zh")]
    one = jnp.int32(1)
    held = jnp.where(is_first, 0, 1)
    index_a = jnp.stack([*at, one, held, one, held]).astype(jnp.int32)
    index_b = jnp.stack([*at, one, held]).astype(jnp.int32)
    ends = jnp.stack([is_first, is_last]).astype(jnp.int32)
    odd = is_odd.astype(jnp.int32).reshape(1)
    local, is_last, is_odd, on_last, index_a, index_b, ends, odd = lax.optimization_barrier(
        (local, is_last, is_odd, on_last, index_a, index_b, ends, odd)
    )
    n = eigenvectors.shape[0] // 2
    stay = jnp.stack([local[0, 1], local[1, 0], local[1, 1], local[2, 0]])
    half = 2 * stay.shape[1]
    before = ring(stay, "zh", 1)
    after = ring(stay, "zh", -1)
    from_next = shifted(local[0, 0], -1)
    from_prior = shifted(local[2, 1], 1)
    far = ring(before, "zh", 1)
    near_a = jnp.concatenate([stay, after, far, before], axis=1)
    moved = jnp.stack([jnp.where(is_last, local[2, 1], from_next), from_prior])
    before = ring(moved, "y", 1)
    after = ring(moved, "y", -1)
    far = ring(moved, "y", 2)
    near_b = jnp.concatenate([moved, after, far, before], axis=1)
    before_a = ring(near_a, "y", 1)
    after_a = ring(near_a, "y", -1)
    give_a0 = before_a[:, :half]
    give_a1 = after_a[:, half:]
    give_a = give_a0, give_a1
    far0_a = ring(give_a[0], "y", 1)
    far1_a = ring(give_a[1], "y", -1)
    before_b = ring(near_b, "zh", 1)
    after_b = ring(near_b, "zh", -1)
    give_b0 = before_b[:, :half]
    give_b1 = after_b[:, half:]
    give_b = after_these(give_b0, give_a), after_these(give_b1, give_a)
    far0_b = ring(give_b[0], "zh", 1)
    far1_b = ring(give_b[1], "zh", -1)
    data = shifted(after_these(eigenvectors[:n], (near_b,)), -1)
    far0_a = after_these(far0_a, give_b)
    parts_a = prepare(True, index_a, near_a, after_a, before_a, far0_a, far1_a)
    parts_b = prepare(False, index_b, after_these(near_b, parts_a), after_b, before_b, far0_b, far1_b)
    step, rest, add = operate(ends, data, eigenvectors, (*parts_a, *parts_b))

    swap = [(0, 1), (1, 0)]
    half = add.shape[0] // 2
    halves = add.reshape(2, half, 7 * n)
    keep = jnp.where(is_odd, halves[1], halves[0])
    give = jnp.where(is_odd, halves[0], halves[1])
    other = lax.ppermute(step, "core", swap)
    got = lax.ppermute(give, "core", swap)
    rest, other, got = lax.optimization_barrier((rest, other, got))
    high, low, chip_add = merge(odd, step, other, keep[:, : 3 * n], got[:, : 3 * n])
    other_rest = lax.ppermute(rest, "core", swap)

    sub = half // SUBS
    adds = [chip_add[k * sub : (k + 1) * sub] for k in range(SUBS)]

    def onward(value, hop):
        return lax.ppermute(value, CHIP, [(hop - 1, hop)])

    arrived = [[onward(part, 1)] for part in adds]
    for hop in range(2, chips):
        for k in range(SUBS):
            sent = hop_on(arrived[k][-1], high, low, adds[k])
            arrived[k].append(onward(sent, hop))
        if hop == 4:
            ended = ending(odd, step, other, after_these(rest, [sent]), other_rest, keep, got)
        if hop == 5:
            for values in arrived:
                values[-1] = after_these(values[-1], ended)
    final = finish(arrived, *ended)
    for_prior, for_even, for_odd = [final[:, 2 * k * n : 2 * (k + 1) * n] for k in range(3)]
    got = lax.ppermute(jnp.where(is_odd, for_even, for_odd), "core", swap)
    handed = [
        lax.ppermute(for_prior, ROW, [(2 * (k + 1) + side, 2 * k + 1) for k in range(chips - 1)]) for side in range(2)
    ]
    got, *handed = lax.optimization_barrier((got, *handed))
    upper = jnp.where(is_odd, jnp.where(on_last, got, handed[0]), for_even)
    lower = jnp.where(is_odd, jnp.where(on_last, for_odd, handed[1]), got)
    return jnp.concatenate([upper, lower], axis=0).T


def solution(mesh):
    split_mesh = Mesh(mesh.devices.reshape(2, 4, 2, 4, 4), (*ROW, *COL))
    return jax.shard_map(
        shards,
        mesh=split_mesh,
        in_specs=(P(ROW, COL), P(None, ROW, None, COL)),
        out_specs=P(ROW, COL),
        check_vma=False,
    )
```

```python
import functools

import jax
import jax.numpy as jnp
from jax import lax
from jax.experimental import pallas as pl
from jax.experimental.pallas import tpu as pltpu
from jax.sharding import Mesh
from jax.sharding import PartitionSpec as P

ROW = ("zl", "x", "core")
CHIP = ("zl", "x")
COL = ("y", "zh")
SUBS = 2
INTERPRET = False

NN = (((1,), (0,)), ((), ()))
NT = (((1,), (1,)), ((), ()))


def split(value):
    high = value.astype(jnp.bfloat16)
    low = (value - high.astype(jnp.float32)).astype(jnp.bfloat16)
    return high, low


def dot3(left, right, dims=NN):
    (on_left,), (on_right,) = dims[0]
    long_left = jnp.concatenate([left[0], left[0], left[1]], axis=on_left)
    long_right = jnp.concatenate([right[0], right[1], right[0]], axis=on_right)
    return lax.dot_general(long_left, long_right, dims, preferred_element_type=jnp.float32)


def prepare_body(outer_y, index_ref, near_ref, after_ref, before_ref, far0_ref, far1_ref, high_ref, low_ref, v_ref, g_ref, p_ref):
    blocks, quarter, m = near_ref.shape
    n = 4 * quarter
    half = n // 2
    piece = quarter // 4
    at_y = index_ref[0]
    at_z = index_ref[1]
    for outer in range(4):
        for inner in range(4):
            dy, dz = (outer, inner) if outer_y else (inner, outer)
            start = lax.rem(at_y + dy, 4) * quarter + lax.rem(at_z + dz, 4) * piece
            at = pl.ds(inner * piece, piece)
            for block in range(blocks):
                if outer == 0:
                    part = near_ref[block, at, :]
                elif outer == 1:
                    part = after_ref[block, at, :]
                elif outer == 3:
                    part = before_ref[block, at, :]
                elif inner < 2:
                    part = far0_ref[block, at, :]
                else:
                    part = far1_ref[block, pl.ds((inner - 2) * piece, piece), :]
                v_ref[block, pl.ds(start, piece), :] = part
    rows = lax.broadcasted_iota(jnp.int32, (half, half), 0)
    cols = lax.broadcasted_iota(jnp.int32, (half, half), 1)
    eye = rows == cols
    pair = (rows // 2 == cols // 2) & (rows < cols)
    for block in range(blocks):
        vectors = split(v_ref[block])
        g_ref[block] = dot3(vectors, vectors, NT)
    problems = [(block, side) for block in range(blocks) for side in range(2)]
    for at, (block, side) in enumerate(problems):
        lo = side * half
        gram = g_ref[block, lo : lo + half, lo : lo + half]
        on_diagonal = jnp.where(eye, gram, 0.0)
        col_inverse = 1.0 / (0.5 * jnp.sum(on_diagonal, axis=1, keepdims=True))
        row_inverse = 1.0 / (0.5 * jnp.sum(on_diagonal, axis=0, keepdims=True))
        inverse = jnp.where(eye, col_inverse, 0.0)
        p_ref[at] = inverse - jnp.where(pair, gram * col_inverse * row_inverse, 0.0)

    levels = half.bit_length() - 1

    def level(power, carry):
        old_rows = jnp.right_shift(rows, power)
        old_cols = jnp.right_shift(cols, power)
        corner = (jnp.right_shift(old_rows, 1) == jnp.right_shift(old_cols, 1)) & (old_rows < old_cols)
        first = []
        for at, (block, side) in enumerate(problems):
            lo = side * half
            edge = split(jnp.where(corner, g_ref[block, lo : lo + half, lo : lo + half], 0.0))
            first.append(dot3(split(p_ref[at]), edge))
        for at in range(len(problems)):
            old = p_ref[at]
            p_ref[at] = old - dot3(split(first[at]), split(old))
        return carry

    lax.fori_loop(1, levels, level, 0)
    eye = lax.broadcasted_iota(jnp.int32, (m, m), 0) == lax.broadcasted_iota(jnp.int32, (m, m), 1)
    unit = jnp.where(eye, 1.0, 0.0)
    first = [
        dot3(split(p_ref[2 * block]), split(g_ref[block, :half, half:])) for block in range(blocks)
    ]
    corners = [dot3(split(first[block]), split(p_ref[2 * block + 1])) for block in range(blocks)]
    for block in range(blocks):
        vectors = split(v_ref[block])
        top = split(jnp.concatenate([p_ref[2 * block], -corners[block]], axis=1))
        low = split(p_ref[2 * block + 1])
        upper = dot3(top, vectors)
        lower = dot3(low, (vectors[0][half:], vectors[1][half:]))
        scaled = split(jnp.concatenate([upper, lower], axis=0).T)
        whole = unit - dot3(scaled, vectors)
        whole = jnp.where(index_ref[2 + block] == 1, whole, unit)
        high, low = split(whole)
        high_ref[block] = high
        low_ref[block] = low


def prepare(outer_y, index, near, after, before, far0, far1):
    blocks, quarter, m = near.shape
    n = 4 * quarter
    out = jax.ShapeDtypeStruct((blocks, m, m), jnp.bfloat16)
    vmem = pl.BlockSpec(memory_space=pltpu.VMEM)
    return pl.pallas_call(
        functools.partial(prepare_body, outer_y),
        out_shape=(out, out),
        in_specs=[pl.BlockSpec(memory_space=pltpu.SMEM)] + [vmem] * 5,
        out_specs=(vmem, vmem),
        scratch_shapes=[
            pltpu.VMEM((blocks, n, m), jnp.float32),
            pltpu.VMEM((blocks, n, n), jnp.float32),
            pltpu.VMEM((2 * blocks, n // 2, n // 2), jnp.float32),
        ],
        compiler_params=pltpu.CompilerParams(vmem_limit_bytes=14 * 1024 * 1024),
        cost_estimate=pl.CostEstimate(flops=2_000_000_000, bytes_accessed=1_000_000, transcendentals=0),
        interpret=INTERPRET,
        name="prepare",
    )(index, near, after, before, far0, far1)


PAIRS = ((0, 0), (0, 1), (0, 2), (1, 1), (1, 2), (2, 2))


def operate_body(ends_ref, data_ref, own_ref, ah, al, bh, bl, step_ref, rest_ref, add_ref):
    n = ah.shape[1] // 2
    first = ends_ref[0] == 1
    last = ends_ref[1] == 1
    width = data_ref.shape[1]
    held = {(0, 0): (ah, al, 0), (0, 1): (bh, bl, 0), (1, 0): (ah, al, 1), (1, 1): (ah, al, 2), (2, 0): (bh, bl, 1), (2, 1): (ah, al, 3)}

    def part(sweep, block, side=None):
        high, low, at = held[sweep, block]
        if side is None:
            return high[at], low[at]
        rows = pl.ds(side * n, n)
        return high[at, rows, :], low[at, rows, :]

    for sweep in range(3):
        a_top = part(sweep, 0, 0)
        b_top = part(sweep, 1, 0)
        b_low = part(sweep, 1, 1)
        fresh = a_top[0].astype(jnp.float32) + a_top[1].astype(jnp.float32)
        if sweep == 0:
            own = own_ref[...].T
            arriving = jnp.where(first, own[:, :n], 0.0)
            mid = dot3(split(jnp.concatenate([arriving, own[:, n:]], axis=1)), part(0, 0))
            mid = jnp.concatenate([fresh, mid], axis=0)
            v = data_ref[...].T
            done = dot3(split(mid[:, n:]), b_top)
            done = jnp.concatenate([done[:n], done[n:] + dot3(split(v), b_low)], axis=0)
            v = jnp.concatenate([jnp.zeros((n, n), jnp.float32), v], axis=0)
            done = jnp.where(last, jnp.concatenate([mid[:, n:], v], axis=1), done)
        else:
            mid = dot3(split(u), part(sweep, 0, 1))
            mid = jnp.concatenate([mid[:-width], fresh, mid[-width:]], axis=0)
            done = dot3(split(mid[:, n:]), b_top)
            more = dot3(split(v), b_low)
            early = sweep * n
            done = jnp.concatenate(
                [done[:early] + more[:early], done[early : early + n], done[early + n :] + more[early:]], axis=0
            )
        known = (sweep + 1) * n
        u, v = mid[:, :n], done[:, :n]
        out = done[:, n:]
        for k in range(sweep + 1):
            step_ref[PAIRS.index((k, sweep))] = out[k * n : (k + 1) * n]
        add_ref[:, sweep * n : (sweep + 1) * n] = out[known:]
    rest_ref[:, 0:n] = u[: 3 * n]
    rest_ref[:, n : 2 * n] = v[: 3 * n]
    add_ref[:, 3 * n : 4 * n] = u[3 * n :]
    add_ref[:, 4 * n : 5 * n] = v[3 * n :]

    @pl.when(last)
    def _():
        high, low = bh[0], bl[0]
        for k in range(4):
            if k < 3:
                upper = step_ref[PAIRS.index((k, 2))]
                lower = step_ref[PAIRS.index((k, 1))] if k < 2 else jnp.zeros((n, n), jnp.float32)
            else:
                upper = add_ref[:, 2 * n : 3 * n]
                lower = add_ref[:, n : 2 * n]
            result = dot3(split(jnp.concatenate([upper, lower], axis=1)), (high, low))
            if k < 3:
                rest_ref[k * n : (k + 1) * n, 2 * n :] = result
            else:
                add_ref[:, 5 * n :] = result

    @pl.when(jnp.logical_not(last))
    def _():
        rest_ref[:, 2 * n :] = jnp.zeros((3 * n, 2 * n), jnp.float32)
        add_ref[:, 5 * n :] = jnp.zeros((width, 2 * n), jnp.float32)


def operate(ends, data, own, parts):
    m, width = own.shape
    n = m // 2
    vmem = pl.BlockSpec(memory_space=pltpu.VMEM)
    return pl.pallas_call(
        operate_body,
        out_shape=(
            jax.ShapeDtypeStruct((6, n, n), jnp.float32),
            jax.ShapeDtypeStruct((3 * n, 4 * n), jnp.float32),
            jax.ShapeDtypeStruct((width, 7 * n), jnp.float32),
        ),
        in_specs=[pl.BlockSpec(memory_space=pltpu.SMEM)] + [vmem] * 6,
        out_specs=(vmem,) * 3,
        compiler_params=pltpu.CompilerParams(vmem_limit_bytes=20 * 1024 * 1024),
        interpret=INTERPRET,
        name="operate",
    )(ends, data, own, *parts)


def merge_body(odd_ref, mine_ref, other_ref, keep_ref, got_ref, high_ref, low_ref, add_ref):
    n = mine_ref.shape[1]
    odd = odd_ref[0] == 1
    keep = keep_ref[...]
    got = got_ref[...]
    even_parts = [split(jnp.where(odd, other_ref[k], mine_ref[k])) for k in range(6)]
    odd_parts = [split(jnp.where(odd, mine_ref[k], other_ref[k])) for k in range(6)]
    odd_add = jnp.where(odd, keep, got)
    add_parts = split(jnp.where(odd, got, keep))
    for s in range(3):
        total = odd_add[:, s * n : (s + 1) * n]
        for j in range(s + 1):
            columns = slice(j * n, (j + 1) * n)
            total = total + dot3((add_parts[0][:, columns], add_parts[1][:, columns]), odd_parts[PAIRS.index((j, s))])
        add_ref[:, s * n : (s + 1) * n] = total
        for k in range(s + 1):
            total = None
            for j in range(k, s + 1):
                term = dot3(even_parts[PAIRS.index((k, j))], odd_parts[PAIRS.index((j, s))])
                total = term if total is None else total + term
            high_ref[PAIRS.index((k, s))], low_ref[PAIRS.index((k, s))] = split(total)


def merge(odd, mine, other, keep, got):
    n = mine.shape[1]
    half = keep.shape[0]
    vmem = pl.BlockSpec(memory_space=pltpu.VMEM)
    packed = jax.ShapeDtypeStruct((6, n, n), jnp.bfloat16)
    return pl.pallas_call(
        merge_body,
        out_shape=(packed, packed, jax.ShapeDtypeStruct((half, 3 * n), jnp.float32)),
        in_specs=[pl.BlockSpec(memory_space=pltpu.SMEM)] + [vmem] * 4,
        out_specs=(vmem,) * 3,
        compiler_params=pltpu.CompilerParams(vmem_limit_bytes=20 * 1024 * 1024),
        interpret=INTERPRET,
        name="merge",
    )(odd, mine, other, keep, got)


def hop_body(state_ref, high_ref, low_ref, add_ref, out_ref):
    n = high_ref.shape[1]
    high, low = split(state_ref[...])
    count = high.shape[0]
    both = jnp.concatenate([high, low], axis=0)
    for s in range(3):
        total = add_ref[:, s * n : (s + 1) * n]
        for k in range(s + 1):
            at = PAIRS.index((k, s))
            columns = slice(k * n, (k + 1) * n)
            main = lax.dot_general(both[:, columns], high_ref[at], NN, preferred_element_type=jnp.float32)
            side = lax.dot_general(high[:, columns], low_ref[at], NN, preferred_element_type=jnp.float32)
            total = total + (main[:count] + (main[count:] + side))
        out_ref[:, s * n : (s + 1) * n] = total


def hop_on(state, high, low, add):
    vmem = pl.BlockSpec(memory_space=pltpu.VMEM)
    return pl.pallas_call(
        hop_body,
        out_shape=jax.ShapeDtypeStruct(state.shape, jnp.float32),
        in_specs=[vmem] * 4,
        out_specs=vmem,
        compiler_params=pltpu.CompilerParams(vmem_limit_bytes=8 * 1024 * 1024),
        interpret=INTERPRET,
        name="hop",
    )(state, high, low, add)


def ending_body(odd_ref, mine_ref, other_ref, rest_ref, other_rest_ref, keep_ref, got_ref, high_ref, low_ref, add_ref):
    n = mine_ref.shape[1]
    odd = odd_ref[0] == 1
    for k in range(3):
        rows = slice(k * n, (k + 1) * n)
        even_rest = jnp.where(odd, other_rest_ref[rows, : 2 * n], rest_ref[rows, : 2 * n])
        high_ref[rows, : 2 * n], low_ref[rows, : 2 * n] = split(even_rest)
    odd_parts = []
    for k in range(3):
        rows = slice(k * n, (k + 1) * n)
        odd_parts.append(split(jnp.where(odd, rest_ref[rows, :], other_rest_ref[rows, :])))
    for k in range(3):
        total = None
        for j in range(k, 3):
            at = PAIRS.index((k, j))
            term = dot3(split(jnp.where(odd, other_ref[at], mine_ref[at])), odd_parts[j])
            total = term if total is None else total + term
        rows = slice(k * n, (k + 1) * n)
        high_ref[rows, 2 * n :], low_ref[rows, 2 * n :] = split(total)
    even_add = jnp.where(odd, got_ref[...], keep_ref[...])
    odd_add = jnp.where(odd, keep_ref[...], got_ref[...])
    total = odd_add[:, 3 * n :]
    for j in range(3):
        total = total + dot3(split(even_add[:, j * n : (j + 1) * n]), odd_parts[j])
    add_ref[:, : 2 * n] = even_add[:, 3 * n : 5 * n]
    add_ref[:, 2 * n :] = total


def ending(odd, mine, other, rest, other_rest, keep, got):
    n = mine.shape[1]
    vmem = pl.BlockSpec(memory_space=pltpu.VMEM)
    wide = jax.ShapeDtypeStruct((3 * n, 6 * n), jnp.bfloat16)
    return pl.pallas_call(
        ending_body,
        out_shape=(wide, wide, jax.ShapeDtypeStruct((keep.shape[0], 6 * n), jnp.float32)),
        in_specs=[pl.BlockSpec(memory_space=pltpu.SMEM)] + [vmem] * 6,
        out_specs=(vmem,) * 3,
        compiler_params=pltpu.CompilerParams(vmem_limit_bytes=16 * 1024 * 1024),
        interpret=INTERPRET,
        name="ending",
    )(odd, mine, other, rest, other_rest, keep, got)


def finish_body(*refs):
    *state_refs, high_ref, low_ref, add_ref, out_ref, sum_ref = refs
    hops = len(state_refs) // SUBS
    width = out_ref.shape[1]
    rows = []
    for k in range(SUBS):
        total = state_refs[k * hops][...]
        for ref in state_refs[k * hops + 1 : (k + 1) * hops]:
            total = total + ref[...]
        rows.append(total)
    state = jnp.concatenate(rows, axis=0)
    sum_ref[...] = state
    out_ref[...] = dot3(split(state), (high_ref[:, :width], low_ref[:, :width])) + add_ref[:, :width]


def finish(arrived, high, low, add):
    vmem = pl.BlockSpec(memory_space=pltpu.VMEM)
    states = [value for values in arrived for value in values]
    return pl.pallas_call(
        finish_body,
        out_shape=(
            jax.ShapeDtypeStruct((add.shape[0], add.shape[1] // 3), jnp.float32),
            jax.ShapeDtypeStruct((add.shape[0], high.shape[0]), jnp.float32),
        ),
        in_specs=[vmem] * (len(states) + 3),
        out_specs=(vmem, vmem),
        compiler_params=pltpu.CompilerParams(vmem_limit_bytes=16 * 1024 * 1024),
        interpret=INTERPRET,
        name="finish",
    )(*states, high, low, add)


def finish_own_body(state_ref, high_ref, low_ref, add_ref, even_ref, odd_ref):
    width = even_ref.shape[1]
    state = split(state_ref[...])
    for k, ref in ((1, even_ref), (2, odd_ref)):
        at = slice(k * width, (k + 1) * width)
        ref[...] = dot3(state, (high_ref[:, at], low_ref[:, at])) + add_ref[:, at]


def finish_own(state, high, low, add):
    vmem = pl.BlockSpec(memory_space=pltpu.VMEM)
    out = jax.ShapeDtypeStruct((add.shape[0], add.shape[1] // 3), jnp.float32)
    return pl.pallas_call(
        finish_own_body,
        out_shape=(out, out),
        in_specs=[vmem] * 4,
        out_specs=(vmem, vmem),
        compiler_params=pltpu.CompilerParams(vmem_limit_bytes=16 * 1024 * 1024),
        interpret=INTERPRET,
        name="finish_own",
    )(state, high, low, add)


def ring(value, axis, step):
    count = lax.axis_size(axis)
    return lax.ppermute(value, axis, [(k, (k + step) % count) for k in range(count)])


def shifted(value, step):
    count = lax.axis_size(ROW)
    return lax.ppermute(value, ROW, [(k, k + step) for k in range(max(0, -step), min(count, count - step))])


def after_these(value, others):
    return lax.optimization_barrier((value, *others))[0]


def shards(eigenvectors, householder):
    local = jnp.swapaxes(householder, 2, 3)
    position = lax.axis_index(ROW)
    count = lax.axis_size(ROW)
    chips = lax.axis_size(CHIP)
    is_first = position == 0
    is_last = position == count - 1
    is_odd = lax.axis_index("core") == 1
    middle = chips // 2
    flipped = lax.axis_index(CHIP) >= middle
    flips_next = lax.axis_index(CHIP) + 1 >= middle
    takes_second = is_odd != flipped
    on_last = lax.axis_index(CHIP) == chips - 1
    at = [lax.axis_index("y"), lax.axis_index("zh")]
    one = jnp.int32(1)
    held = jnp.where(is_first, 0, 1)
    index_a = jnp.stack([*at, one, held, one, held]).astype(jnp.int32)
    index_b = jnp.stack([*at, one, held]).astype(jnp.int32)
    ends = jnp.stack([is_first, is_last]).astype(jnp.int32)
    odd = is_odd.astype(jnp.int32).reshape(1)
    local, is_last, is_odd, flipped, flips_next, takes_second, on_last, index_a, index_b, ends, odd = lax.optimization_barrier(
        (local, is_last, is_odd, flipped, flips_next, takes_second, on_last, index_a, index_b, ends, odd)
    )
    n = eigenvectors.shape[0] // 2
    stay = jnp.stack([local[0, 1], local[1, 0], local[1, 1], local[2, 0]])
    half = 2 * stay.shape[1]
    before = ring(stay, "zh", 1)
    after = ring(stay, "zh", -1)
    from_next = shifted(local[0, 0], -1)
    from_prior = shifted(local[2, 1], 1)
    far = ring(before, "zh", 1)
    near_a = jnp.concatenate([stay, after, far, before], axis=1)
    moved = jnp.stack([jnp.where(is_last, local[2, 1], from_next), from_prior])
    before = ring(moved, "y", 1)
    after = ring(moved, "y", -1)
    far = ring(moved, "y", 2)
    near_b = jnp.concatenate([moved, after, far, before], axis=1)
    before_a = ring(near_a, "y", 1)
    after_a = ring(near_a, "y", -1)
    give_a0 = before_a[:, :half]
    give_a1 = after_a[:, half:]
    give_a = give_a0, give_a1
    far0_a = ring(give_a[0], "y", 1)
    far1_a = ring(give_a[1], "y", -1)
    before_b = ring(near_b, "zh", 1)
    after_b = ring(near_b, "zh", -1)
    give_b0 = before_b[:, :half]
    give_b1 = after_b[:, half:]
    give_b = after_these(give_b0, give_a), after_these(give_b1, give_a)
    far0_b = ring(give_b[0], "zh", 1)
    far1_b = ring(give_b[1], "zh", -1)
    data = shifted(after_these(eigenvectors[:n], (near_b,)), -1)
    far0_a = after_these(far0_a, give_b)
    parts_a = prepare(True, index_a, near_a, after_a, before_a, far0_a, far1_a)
    parts_b = prepare(False, index_b, after_these(near_b, parts_a), after_b, before_b, far0_b, far1_b)
    step, rest, add = operate(ends, data, eigenvectors, (*parts_a, *parts_b))

    swap = [(0, 1), (1, 0)]
    half = add.shape[0] // 2
    halves = add.reshape(2, half, 7 * n)
    keep = jnp.where(takes_second, halves[1], halves[0])
    give = jnp.where(takes_second, halves[0], halves[1])
    other = lax.ppermute(step, "core", swap)
    got = lax.ppermute(give, "core", swap)
    rest, other, got = lax.optimization_barrier((rest, other, got))
    high, low, chip_add = merge(odd, step, other, keep[:, : 3 * n], got[:, : 3 * n])
    other_rest = lax.ppermute(rest, "core", swap)

    sub = half // SUBS
    adds = [chip_add[k * sub : (k + 1) * sub] for k in range(SUBS)]

    def onward(value, hop):
        turn = 1 if hop == middle else 0
        return lax.ppermute(value, ROW, [(2 * hop - 2 + side, 2 * hop + (side ^ turn)) for side in range(2)])

    arrived = [[onward(part, 1)] for part in adds]
    for hop in range(2, chips):
        for k in range(SUBS):
            sent = hop_on(arrived[k][-1], high, low, adds[k])
            arrived[k].append(onward(sent, hop))
        if hop == 4:
            ended = ending(odd, step, other, after_these(rest, [sent]), other_rest, keep, got)
        if hop == 5:
            for values in arrived:
                values[-1] = after_these(values[-1], ended)
    for_prior, state = finish(arrived, *ended)
    handed = []
    for side in range(2):
        pairs = [(2 * (k + 1) + side, 2 * k + 1) for k in range(chips - 1)]
        handed.append(lax.ppermute(for_prior, ROW, pairs))
    for_even, for_odd = finish_own(state, *ended)
    got = lax.ppermute(jnp.where(is_odd, for_even, for_odd), "core", swap)
    got, *handed = lax.optimization_barrier((got, *handed))
    near, far = jnp.where(flips_next, handed[1], handed[0]), jnp.where(flips_next, handed[0], handed[1])
    upper = jnp.where(is_odd, jnp.where(on_last, for_odd, near), jnp.where(flipped, got, for_even))
    lower = jnp.where(is_odd, jnp.where(on_last, got, far), jnp.where(flipped, for_even, got))
    return jnp.concatenate([upper, lower], axis=0).T


def solution(mesh):
    split_mesh = Mesh(mesh.devices.reshape(2, 4, 2, 4, 4), (*ROW, *COL))
    return jax.shard_map(
        shards,
        mesh=split_mesh,
        in_specs=(P(ROW, COL), P(None, ROW, None, COL)),
        out_specs=P(ROW, COL),
        check_vma=False,
    )
```

```python
import functools

import jax
import jax.numpy as jnp
from jax import lax
from jax.experimental import pallas as pl
from jax.experimental.pallas import tpu as pltpu
from jax.sharding import Mesh
from jax.sharding import PartitionSpec as P

ROW = ("zl", "x", "core")
CHIP = ("zl", "x")
COL = ("y", "zh")
SUBS = 2
INTERPRET = False

NN = (((1,), (0,)), ((), ()))
NT = (((1,), (1,)), ((), ()))


def split(value):
    high = value.astype(jnp.bfloat16)
    low = (value - high.astype(jnp.float32)).astype(jnp.bfloat16)
    return high, low


def dot3(left, right, dims=NN):
    (on_left,), (on_right,) = dims[0]
    long_left = jnp.concatenate([left[0], left[0], left[1]], axis=on_left)
    long_right = jnp.concatenate([right[0], right[1], right[0]], axis=on_right)
    return lax.dot_general(long_left, long_right, dims, preferred_element_type=jnp.float32)


def prepare_body(outer_y, index_ref, near_ref, after_ref, before_ref, far0_ref, far1_ref, high_ref, low_ref, v_ref, g_ref, p_ref):
    blocks, quarter, m = near_ref.shape
    n = 4 * quarter
    half = n // 2
    piece = quarter // 4
    at_y = index_ref[0]
    at_z = index_ref[1]
    for outer in range(4):
        for inner in range(4):
            dy, dz = (outer, inner) if outer_y else (inner, outer)
            start = lax.rem(at_y + dy, 4) * quarter + lax.rem(at_z + dz, 4) * piece
            at = pl.ds(inner * piece, piece)
            for block in range(blocks):
                if outer == 0:
                    part = near_ref[block, at, :]
                elif outer == 1:
                    part = after_ref[block, at, :]
                elif outer == 3:
                    part = before_ref[block, at, :]
                elif inner < 2:
                    part = far0_ref[block, at, :]
                else:
                    part = far1_ref[block, pl.ds((inner - 2) * piece, piece), :]
                v_ref[block, pl.ds(start, piece), :] = part
    rows = lax.broadcasted_iota(jnp.int32, (half, half), 0)
    cols = lax.broadcasted_iota(jnp.int32, (half, half), 1)
    eye = rows == cols
    pair = (rows // 2 == cols // 2) & (rows < cols)
    for block in range(blocks):
        vectors = split(v_ref[block])
        g_ref[block] = dot3(vectors, vectors, NT)
    problems = [(block, side) for block in range(blocks) for side in range(2)]
    for at, (block, side) in enumerate(problems):
        lo = side * half
        gram = g_ref[block, lo : lo + half, lo : lo + half]
        on_diagonal = jnp.where(eye, gram, 0.0)
        col_inverse = 1.0 / (0.5 * jnp.sum(on_diagonal, axis=1, keepdims=True))
        row_inverse = 1.0 / (0.5 * jnp.sum(on_diagonal, axis=0, keepdims=True))
        inverse = jnp.where(eye, col_inverse, 0.0)
        p_ref[at] = inverse - jnp.where(pair, gram * col_inverse * row_inverse, 0.0)

    levels = half.bit_length() - 1

    def level(power, carry):
        old_rows = jnp.right_shift(rows, power)
        old_cols = jnp.right_shift(cols, power)
        corner = (jnp.right_shift(old_rows, 1) == jnp.right_shift(old_cols, 1)) & (old_rows < old_cols)
        first = []
        for at, (block, side) in enumerate(problems):
            lo = side * half
            edge = split(jnp.where(corner, g_ref[block, lo : lo + half, lo : lo + half], 0.0))
            first.append(dot3(split(p_ref[at]), edge))
        for at in range(len(problems)):
            old = p_ref[at]
            p_ref[at] = old - dot3(split(first[at]), split(old))
        return carry

    lax.fori_loop(1, levels, level, 0)
    eye = lax.broadcasted_iota(jnp.int32, (m, m), 0) == lax.broadcasted_iota(jnp.int32, (m, m), 1)
    unit = jnp.where(eye, 1.0, 0.0)
    first = [
        dot3(split(p_ref[2 * block]), split(g_ref[block, :half, half:])) for block in range(blocks)
    ]
    corners = [dot3(split(first[block]), split(p_ref[2 * block + 1])) for block in range(blocks)]
    for block in range(blocks):
        vectors = split(v_ref[block])
        top = split(jnp.concatenate([p_ref[2 * block], -corners[block]], axis=1))
        low = split(p_ref[2 * block + 1])
        upper = dot3(top, vectors)
        lower = dot3(low, (vectors[0][half:], vectors[1][half:]))
        scaled = split(jnp.concatenate([upper, lower], axis=0).T)
        whole = unit - dot3(scaled, vectors)
        whole = jnp.where(index_ref[2 + block] == 1, whole, unit)
        high, low = split(whole)
        high_ref[block] = high
        low_ref[block] = low


def prepare(outer_y, index, near, after, before, far0, far1):
    blocks, quarter, m = near.shape
    n = 4 * quarter
    out = jax.ShapeDtypeStruct((blocks, m, m), jnp.bfloat16)
    vmem = pl.BlockSpec(memory_space=pltpu.VMEM)
    return pl.pallas_call(
        functools.partial(prepare_body, outer_y),
        out_shape=(out, out),
        in_specs=[pl.BlockSpec(memory_space=pltpu.SMEM)] + [vmem] * 5,
        out_specs=(vmem, vmem),
        scratch_shapes=[
            pltpu.VMEM((blocks, n, m), jnp.float32),
            pltpu.VMEM((blocks, n, n), jnp.float32),
            pltpu.VMEM((2 * blocks, n // 2, n // 2), jnp.float32),
        ],
        compiler_params=pltpu.CompilerParams(vmem_limit_bytes=14 * 1024 * 1024),
        cost_estimate=pl.CostEstimate(flops=2_000_000_000, bytes_accessed=1_000_000, transcendentals=0),
        interpret=INTERPRET,
        name="prepare",
    )(index, near, after, before, far0, far1)


PAIRS = ((0, 0), (0, 1), (0, 2), (1, 1), (1, 2), (2, 2))


def operate_body(ends_ref, data_ref, own_ref, ah, al, bh, bl, step_ref, rest_ref, add_ref):
    n = ah.shape[1] // 2
    first = ends_ref[0] == 1
    last = ends_ref[1] == 1
    width = data_ref.shape[1]
    held = {(0, 0): (ah, al, 0), (0, 1): (bh, bl, 0), (1, 0): (ah, al, 1), (1, 1): (ah, al, 2), (2, 0): (bh, bl, 1), (2, 1): (ah, al, 3)}

    def part(sweep, block, side=None):
        high, low, at = held[sweep, block]
        if side is None:
            return high[at], low[at]
        rows = pl.ds(side * n, n)
        return high[at, rows, :], low[at, rows, :]

    for sweep in range(3):
        a_top = part(sweep, 0, 0)
        b_top = part(sweep, 1, 0)
        b_low = part(sweep, 1, 1)
        fresh = a_top[0].astype(jnp.float32) + a_top[1].astype(jnp.float32)
        if sweep == 0:
            own = own_ref[...].T
            arriving = jnp.where(first, own[:, :n], 0.0)
            mid = dot3(split(jnp.concatenate([arriving, own[:, n:]], axis=1)), part(0, 0))
            mid = jnp.concatenate([fresh, mid], axis=0)
            v = data_ref[...].T
            done = dot3(split(mid[:, n:]), b_top)
            done = jnp.concatenate([done[:n], done[n:] + dot3(split(v), b_low)], axis=0)
            v = jnp.concatenate([jnp.zeros((n, n), jnp.float32), v], axis=0)
            done = jnp.where(last, jnp.concatenate([mid[:, n:], v], axis=1), done)
        else:
            mid = dot3(split(u), part(sweep, 0, 1))
            mid = jnp.concatenate([mid[:-width], fresh, mid[-width:]], axis=0)
            done = dot3(split(mid[:, n:]), b_top)
            more = dot3(split(v), b_low)
            early = sweep * n
            done = jnp.concatenate(
                [done[:early] + more[:early], done[early : early + n], done[early + n :] + more[early:]], axis=0
            )
        known = (sweep + 1) * n
        u, v = mid[:, :n], done[:, :n]
        out = done[:, n:]
        for k in range(sweep + 1):
            step_ref[PAIRS.index((k, sweep))] = out[k * n : (k + 1) * n]
        add_ref[:, sweep * n : (sweep + 1) * n] = out[known:]
    rest_ref[:, 0:n] = u[: 3 * n]
    rest_ref[:, n : 2 * n] = v[: 3 * n]
    add_ref[:, 3 * n : 4 * n] = u[3 * n :]
    add_ref[:, 4 * n : 5 * n] = v[3 * n :]

    @pl.when(last)
    def _():
        high, low = bh[0], bl[0]
        for k in range(4):
            if k < 3:
                upper = step_ref[PAIRS.index((k, 2))]
                lower = step_ref[PAIRS.index((k, 1))] if k < 2 else jnp.zeros((n, n), jnp.float32)
            else:
                upper = add_ref[:, 2 * n : 3 * n]
                lower = add_ref[:, n : 2 * n]
            result = dot3(split(jnp.concatenate([upper, lower], axis=1)), (high, low))
            if k < 3:
                rest_ref[k * n : (k + 1) * n, 2 * n :] = result
            else:
                add_ref[:, 5 * n :] = result

    @pl.when(jnp.logical_not(last))
    def _():
        rest_ref[:, 2 * n :] = jnp.zeros((3 * n, 2 * n), jnp.float32)
        add_ref[:, 5 * n :] = jnp.zeros((width, 2 * n), jnp.float32)


def operate(ends, data, own, parts):
    m, width = own.shape
    n = m // 2
    vmem = pl.BlockSpec(memory_space=pltpu.VMEM)
    return pl.pallas_call(
        operate_body,
        out_shape=(
            jax.ShapeDtypeStruct((6, n, n), jnp.float32),
            jax.ShapeDtypeStruct((3 * n, 4 * n), jnp.float32),
            jax.ShapeDtypeStruct((width, 7 * n), jnp.float32),
        ),
        in_specs=[pl.BlockSpec(memory_space=pltpu.SMEM)] + [vmem] * 6,
        out_specs=(vmem,) * 3,
        compiler_params=pltpu.CompilerParams(vmem_limit_bytes=20 * 1024 * 1024),
        interpret=INTERPRET,
        name="operate",
    )(ends, data, own, *parts)


def merge_add_body(odd_ref, mine_ref, other_ref, keep_ref, got_ref, add_ref):
    n = mine_ref.shape[1]
    odd = odd_ref[0] == 1
    wide = slice(0, 3 * n)
    keep = keep_ref[:, wide]
    got = got_ref[:, wide]
    odd_parts = [split(jnp.where(odd, mine_ref[k], other_ref[k])) for k in range(6)]
    odd_add = jnp.where(odd, keep, got)
    add_parts = split(jnp.where(odd, got, keep))
    for s in range(3):
        total = odd_add[:, s * n : (s + 1) * n]
        for j in range(s + 1):
            columns = slice(j * n, (j + 1) * n)
            total = total + dot3((add_parts[0][:, columns], add_parts[1][:, columns]), odd_parts[PAIRS.index((j, s))])
        add_ref[:, s * n : (s + 1) * n] = total


def merge_add(odd, mine, other, keep, got):
    n = mine.shape[1]
    vmem = pl.BlockSpec(memory_space=pltpu.VMEM)
    return pl.pallas_call(
        merge_add_body,
        out_shape=jax.ShapeDtypeStruct((keep.shape[0], 3 * n), jnp.float32),
        in_specs=[pl.BlockSpec(memory_space=pltpu.SMEM)] + [vmem] * 4,
        out_specs=vmem,
        compiler_params=pltpu.CompilerParams(vmem_limit_bytes=16 * 1024 * 1024),
        interpret=INTERPRET,
        name="merge_add",
    )(odd, mine, other, keep, got)


def merge_map_body(odd_ref, mine_ref, other_ref, high_ref, low_ref):
    odd = odd_ref[0] == 1
    even_parts = [split(jnp.where(odd, other_ref[k], mine_ref[k])) for k in range(6)]
    odd_parts = [split(jnp.where(odd, mine_ref[k], other_ref[k])) for k in range(6)]
    for s in range(3):
        for k in range(s + 1):
            total = None
            for j in range(k, s + 1):
                term = dot3(even_parts[PAIRS.index((k, j))], odd_parts[PAIRS.index((j, s))])
                total = term if total is None else total + term
            high_ref[PAIRS.index((k, s))], low_ref[PAIRS.index((k, s))] = split(total)


def merge_map(odd, mine, other):
    vmem = pl.BlockSpec(memory_space=pltpu.VMEM)
    packed = jax.ShapeDtypeStruct(mine.shape, jnp.bfloat16)
    return pl.pallas_call(
        merge_map_body,
        out_shape=(packed, packed),
        in_specs=[pl.BlockSpec(memory_space=pltpu.SMEM)] + [vmem] * 2,
        out_specs=(vmem,) * 2,
        compiler_params=pltpu.CompilerParams(vmem_limit_bytes=16 * 1024 * 1024),
        interpret=INTERPRET,
        name="merge_map",
    )(odd, mine, other)


def hop_body(state_ref, high_ref, low_ref, add_ref, out_ref):
    n = high_ref.shape[1]
    high, low = split(state_ref[...])
    count = high.shape[0]
    both = jnp.concatenate([high, low], axis=0)
    for s in range(3):
        total = add_ref[:, s * n : (s + 1) * n]
        for k in range(s + 1):
            at = PAIRS.index((k, s))
            columns = slice(k * n, (k + 1) * n)
            main = lax.dot_general(both[:, columns], high_ref[at], NN, preferred_element_type=jnp.float32)
            side = lax.dot_general(high[:, columns], low_ref[at], NN, preferred_element_type=jnp.float32)
            total = total + (main[:count] + (main[count:] + side))
        out_ref[:, s * n : (s + 1) * n] = total


def hop_on(state, high, low, add):
    vmem = pl.BlockSpec(memory_space=pltpu.VMEM)
    return pl.pallas_call(
        hop_body,
        out_shape=jax.ShapeDtypeStruct(state.shape, jnp.float32),
        in_specs=[vmem] * 4,
        out_specs=vmem,
        compiler_params=pltpu.CompilerParams(vmem_limit_bytes=8 * 1024 * 1024),
        interpret=INTERPRET,
        name="hop",
    )(state, high, low, add)


def ending_body(odd_ref, mine_ref, other_ref, rest_ref, other_rest_ref, keep_ref, got_ref, high_ref, low_ref, add_ref):
    n = mine_ref.shape[1]
    odd = odd_ref[0] == 1
    for k in range(3):
        rows = slice(k * n, (k + 1) * n)
        even_rest = jnp.where(odd, other_rest_ref[rows, : 2 * n], rest_ref[rows, : 2 * n])
        high_ref[rows, : 2 * n], low_ref[rows, : 2 * n] = split(even_rest)
    odd_parts = []
    for k in range(3):
        rows = slice(k * n, (k + 1) * n)
        odd_parts.append(split(jnp.where(odd, rest_ref[rows, :], other_rest_ref[rows, :])))
    for k in range(3):
        total = None
        for j in range(k, 3):
            at = PAIRS.index((k, j))
            term = dot3(split(jnp.where(odd, other_ref[at], mine_ref[at])), odd_parts[j])
            total = term if total is None else total + term
        rows = slice(k * n, (k + 1) * n)
        high_ref[rows, 2 * n :], low_ref[rows, 2 * n :] = split(total)
    even_add = jnp.where(odd, got_ref[...], keep_ref[...])
    odd_add = jnp.where(odd, keep_ref[...], got_ref[...])
    total = odd_add[:, 3 * n :]
    for j in range(3):
        total = total + dot3(split(even_add[:, j * n : (j + 1) * n]), odd_parts[j])
    add_ref[:, : 2 * n] = even_add[:, 3 * n : 5 * n]
    add_ref[:, 2 * n :] = total


def ending(odd, mine, other, rest, other_rest, keep, got):
    n = mine.shape[1]
    vmem = pl.BlockSpec(memory_space=pltpu.VMEM)
    wide = jax.ShapeDtypeStruct((3 * n, 6 * n), jnp.bfloat16)
    return pl.pallas_call(
        ending_body,
        out_shape=(wide, wide, jax.ShapeDtypeStruct((keep.shape[0], 6 * n), jnp.float32)),
        in_specs=[pl.BlockSpec(memory_space=pltpu.SMEM)] + [vmem] * 6,
        out_specs=(vmem,) * 3,
        compiler_params=pltpu.CompilerParams(vmem_limit_bytes=16 * 1024 * 1024),
        interpret=INTERPRET,
        name="ending",
    )(odd, mine, other, rest, other_rest, keep, got)


def finish_body(*refs):
    *state_refs, high_ref, low_ref, add_ref, out_ref, sum_ref = refs
    hops = len(state_refs) // SUBS
    width = out_ref.shape[1]
    rows = []
    for k in range(SUBS):
        total = state_refs[k * hops][...]
        for ref in state_refs[k * hops + 1 : (k + 1) * hops]:
            total = total + ref[...]
        rows.append(total)
    state = jnp.concatenate(rows, axis=0)
    sum_ref[...] = state
    out_ref[...] = dot3(split(state), (high_ref[:, :width], low_ref[:, :width])) + add_ref[:, :width]


def finish(arrived, high, low, add):
    vmem = pl.BlockSpec(memory_space=pltpu.VMEM)
    states = [value for values in arrived for value in values]
    return pl.pallas_call(
        finish_body,
        out_shape=(
            jax.ShapeDtypeStruct((add.shape[0], add.shape[1] // 3), jnp.float32),
            jax.ShapeDtypeStruct((add.shape[0], high.shape[0]), jnp.float32),
        ),
        in_specs=[vmem] * (len(states) + 3),
        out_specs=(vmem, vmem),
        compiler_params=pltpu.CompilerParams(vmem_limit_bytes=16 * 1024 * 1024),
        interpret=INTERPRET,
        name="finish",
    )(*states, high, low, add)


def finish_own_body(state_ref, high_ref, low_ref, add_ref, even_ref, odd_ref):
    width = even_ref.shape[1]
    state = split(state_ref[...])
    for k, ref in ((1, even_ref), (2, odd_ref)):
        at = slice(k * width, (k + 1) * width)
        ref[...] = dot3(state, (high_ref[:, at], low_ref[:, at])) + add_ref[:, at]


def finish_own(state, high, low, add):
    vmem = pl.BlockSpec(memory_space=pltpu.VMEM)
    out = jax.ShapeDtypeStruct((add.shape[0], add.shape[1] // 3), jnp.float32)
    return pl.pallas_call(
        finish_own_body,
        out_shape=(out, out),
        in_specs=[vmem] * 4,
        out_specs=(vmem, vmem),
        compiler_params=pltpu.CompilerParams(vmem_limit_bytes=16 * 1024 * 1024),
        interpret=INTERPRET,
        name="finish_own",
    )(state, high, low, add)


def close_body(places_ref, got_ref, hand0_ref, hand1_ref, even_ref, odd_ref, out_ref):
    odd, last, flipped, flips_next = [places_ref[k] == 1 for k in range(4)]
    got = got_ref[...]
    for_even = even_ref[...]
    for_odd = odd_ref[...]
    near = jnp.where(flips_next, hand1_ref[...], hand0_ref[...])
    far = jnp.where(flips_next, hand0_ref[...], hand1_ref[...])
    upper = jnp.where(odd, jnp.where(last, for_odd, near), jnp.where(flipped, got, for_even))
    lower = jnp.where(odd, jnp.where(last, got, far), jnp.where(flipped, for_even, got))
    out_ref[...] = jnp.concatenate([upper, lower], axis=0).T


def close(places, got, hand0, hand1, for_even, for_odd):
    half, m = got.shape
    vmem = pl.BlockSpec(memory_space=pltpu.VMEM)
    return pl.pallas_call(
        close_body,
        out_shape=jax.ShapeDtypeStruct((m, 2 * half), jnp.float32),
        in_specs=[pl.BlockSpec(memory_space=pltpu.SMEM)] + [vmem] * 5,
        out_specs=vmem,
        compiler_params=pltpu.CompilerParams(vmem_limit_bytes=8 * 1024 * 1024),
        interpret=INTERPRET,
        name="close",
    )(places, got, hand0, hand1, for_even, for_odd)


def ring(value, axis, step):
    count = lax.axis_size(axis)
    return lax.ppermute(value, axis, [(k, (k + step) % count) for k in range(count)])


def shifted(value, step):
    count = lax.axis_size(ROW)
    return lax.ppermute(value, ROW, [(k, k + step) for k in range(max(0, -step), min(count, count - step))])


def after_these(value, others):
    return lax.optimization_barrier((value, *others))[0]


def shards(eigenvectors, householder):
    local = jnp.swapaxes(householder, 2, 3)
    position = lax.axis_index(ROW)
    count = lax.axis_size(ROW)
    chips = lax.axis_size(CHIP)
    is_first = position == 0
    is_last = position == count - 1
    is_odd = lax.axis_index("core") == 1
    middle = chips // 2
    flipped = lax.axis_index(CHIP) >= middle
    flips_next = lax.axis_index(CHIP) + 1 >= middle
    takes_second = is_odd != flipped
    on_last = lax.axis_index(CHIP) == chips - 1
    at = [lax.axis_index("y"), lax.axis_index("zh")]
    one = jnp.int32(1)
    held = jnp.where(is_first, 0, 1)
    index_a = jnp.stack([*at, one, held, one, held]).astype(jnp.int32)
    index_b = jnp.stack([*at, one, held]).astype(jnp.int32)
    ends = jnp.stack([is_first, is_last]).astype(jnp.int32)
    odd = is_odd.astype(jnp.int32).reshape(1)
    places = jnp.stack([is_odd, on_last, flipped, flips_next]).astype(jnp.int32)
    local, is_last, is_odd, takes_second, places, index_a, index_b, ends, odd = lax.optimization_barrier(
        (local, is_last, is_odd, takes_second, places, index_a, index_b, ends, odd)
    )
    n = eigenvectors.shape[0] // 2
    stay = jnp.stack([local[0, 1], local[1, 0], local[1, 1], local[2, 0]])
    half = 2 * stay.shape[1]
    before = ring(stay, "zh", 1)
    after = ring(stay, "zh", -1)
    from_next = shifted(local[0, 0], -1)
    from_prior = shifted(local[2, 1], 1)
    far = ring(before, "zh", 1)
    near_a = jnp.concatenate([stay, after, far, before], axis=1)
    moved = jnp.stack([jnp.where(is_last, local[2, 1], from_next), from_prior])
    before = ring(moved, "y", 1)
    after = ring(moved, "y", -1)
    far = ring(moved, "y", 2)
    near_b = jnp.concatenate([moved, after, far, before], axis=1)
    before_a = ring(near_a, "y", 1)
    after_a = ring(near_a, "y", -1)
    give_a0 = before_a[:, :half]
    give_a1 = after_a[:, half:]
    give_a = give_a0, give_a1
    far0_a = ring(give_a[0], "y", 1)
    far1_a = ring(give_a[1], "y", -1)
    before_b = ring(near_b, "zh", 1)
    after_b = ring(near_b, "zh", -1)
    give_b0 = before_b[:, :half]
    give_b1 = after_b[:, half:]
    give_b = after_these(give_b0, give_a), after_these(give_b1, give_a)
    far0_b = ring(give_b[0], "zh", 1)
    far1_b = ring(give_b[1], "zh", -1)
    data = shifted(after_these(eigenvectors[:n], (near_b,)), -1)
    far0_a = after_these(far0_a, give_b)
    parts_a = prepare(True, index_a, near_a, after_a, before_a, far0_a, far1_a)
    parts_b = prepare(False, index_b, after_these(near_b, parts_a), after_b, before_b, far0_b, far1_b)
    step, rest, add = operate(ends, data, eigenvectors, (*parts_a, *parts_b))

    swap = [(0, 1), (1, 0)]
    half = add.shape[0] // 2
    halves = add.reshape(2, half, 7 * n)
    keep = jnp.where(takes_second, halves[1], halves[0])
    give = jnp.where(takes_second, halves[0], halves[1])
    other = lax.ppermute(step, "core", swap)
    got = lax.ppermute(give, "core", swap)
    rest, other, got = lax.optimization_barrier((rest, other, got))
    chip_add = merge_add(odd, step, other, keep, got)
    other_rest = lax.ppermute(rest, "core", swap)
    high, low = merge_map(odd, step, other)

    sub = half // SUBS
    adds = [chip_add[k * sub : (k + 1) * sub] for k in range(SUBS)]

    def onward(value, hop):
        turn = 1 if hop == middle else 0
        return lax.ppermute(value, ROW, [(2 * hop - 2 + side, 2 * hop + (side ^ turn)) for side in range(2)])

    arrived = []
    for k in range(SUBS):
        arrived.append([onward(adds[k], 1)])
    for hop in range(2, chips):
        for k in range(SUBS):
            sent = hop_on(arrived[k][-1], high, low, adds[k])
            arrived[k].append(onward(sent, hop))
        if hop == 4:
            ended = ending(odd, step, other, after_these(rest, [sent]), other_rest, keep, got)
        if hop == 5:
            for values in arrived:
                values[-1] = after_these(values[-1], ended)
    for_prior, state = finish(arrived, *ended)
    handed = []
    for side in range(2):
        pairs = [(2 * (k + 1) + side, 2 * k + 1) for k in range(chips - 1)]
        handed.append(lax.ppermute(for_prior, ROW, pairs))
    for_even, for_odd = finish_own(state, *ended)
    got = lax.ppermute(jnp.where(is_odd, for_even, for_odd), "core", swap)
    return close(places, got, *handed, for_even, for_odd)


def solution(mesh):
    split_mesh = Mesh(mesh.devices.reshape(2, 4, 2, 4, 4), (*ROW, *COL))
    return jax.shard_map(
        shards,
        mesh=split_mesh,
        in_specs=(P(ROW, COL), P(None, ROW, None, COL)),
        out_specs=P(ROW, COL),
        check_vma=False,
    )
```

```python
import functools

import jax
import jax.numpy as jnp
from jax import lax
from jax.experimental import pallas as pl
from jax.experimental.pallas import tpu as pltpu
from jax.sharding import Mesh
from jax.sharding import PartitionSpec as P

ROW = ("zl", "x", "core")
CHIP = ("zl", "x")
COL = ("y", "zh")
SUBS = 2
INTERPRET = False

NN = (((1,), (0,)), ((), ()))
NT = (((1,), (1,)), ((), ()))


def split(value):
    high = value.astype(jnp.bfloat16)
    low = (value - high.astype(jnp.float32)).astype(jnp.bfloat16)
    return high, low


def dot3(left, right, dims=NN):
    (on_left,), (on_right,) = dims[0]
    long_left = jnp.concatenate([left[0], left[0], left[1]], axis=on_left)
    long_right = jnp.concatenate([right[0], right[1], right[0]], axis=on_right)
    return lax.dot_general(long_left, long_right, dims, preferred_element_type=jnp.float32)


def prepare_body(outer_y, index_ref, near_ref, after_ref, before_ref, far0_ref, far1_ref, high_ref, low_ref, v_ref, g_ref, p_ref):
    blocks, quarter, m = near_ref.shape
    n = 4 * quarter
    half = n // 2
    piece = quarter // 4
    at_y = index_ref[0]
    at_z = index_ref[1]
    for outer in range(4):
        for inner in range(4):
            dy, dz = (outer, inner) if outer_y else (inner, outer)
            start = lax.rem(at_y + dy, 4) * quarter + lax.rem(at_z + dz, 4) * piece
            at = pl.ds(inner * piece, piece)
            for block in range(blocks):
                if outer == 0:
                    part = near_ref[block, at, :]
                elif outer == 1:
                    part = after_ref[block, at, :]
                elif outer == 3:
                    part = before_ref[block, at, :]
                elif inner < 2:
                    part = far0_ref[block, at, :]
                else:
                    part = far1_ref[block, pl.ds((inner - 2) * piece, piece), :]
                v_ref[block, pl.ds(start, piece), :] = part
    rows = lax.broadcasted_iota(jnp.int32, (half, half), 0)
    cols = lax.broadcasted_iota(jnp.int32, (half, half), 1)
    eye = rows == cols
    pair = (rows // 2 == cols // 2) & (rows < cols)
    for block in range(blocks):
        vectors = split(v_ref[block])
        g_ref[block] = dot3(vectors, vectors, NT)
    problems = [(block, side) for block in range(blocks) for side in range(2)]
    for at, (block, side) in enumerate(problems):
        lo = side * half
        gram = g_ref[block, lo : lo + half, lo : lo + half]
        on_diagonal = jnp.where(eye, gram, 0.0)
        col_inverse = 1.0 / (0.5 * jnp.sum(on_diagonal, axis=1, keepdims=True))
        row_inverse = 1.0 / (0.5 * jnp.sum(on_diagonal, axis=0, keepdims=True))
        inverse = jnp.where(eye, col_inverse, 0.0)
        p_ref[at] = inverse - jnp.where(pair, gram * col_inverse * row_inverse, 0.0)

    levels = half.bit_length() - 1

    def level(power, carry):
        old_rows = jnp.right_shift(rows, power)
        old_cols = jnp.right_shift(cols, power)
        corner = (jnp.right_shift(old_rows, 1) == jnp.right_shift(old_cols, 1)) & (old_rows < old_cols)
        first = []
        for at, (block, side) in enumerate(problems):
            lo = side * half
            edge = split(jnp.where(corner, g_ref[block, lo : lo + half, lo : lo + half], 0.0))
            first.append(dot3(split(p_ref[at]), edge))
        for at in range(len(problems)):
            old = p_ref[at]
            p_ref[at] = old - dot3(split(first[at]), split(old))
        return carry

    lax.fori_loop(1, levels, level, 0)
    eye = lax.broadcasted_iota(jnp.int32, (m, m), 0) == lax.broadcasted_iota(jnp.int32, (m, m), 1)
    unit = jnp.where(eye, 1.0, 0.0)
    first = [
        dot3(split(p_ref[2 * block]), split(g_ref[block, :half, half:])) for block in range(blocks)
    ]
    corners = [dot3(split(first[block]), split(p_ref[2 * block + 1])) for block in range(blocks)]
    for block in range(blocks):
        vectors = split(v_ref[block])
        top = split(jnp.concatenate([p_ref[2 * block], -corners[block]], axis=1))
        low = split(p_ref[2 * block + 1])
        upper = dot3(top, vectors)
        lower = dot3(low, (vectors[0][half:], vectors[1][half:]))
        scaled = split(jnp.concatenate([upper, lower], axis=0).T)
        whole = unit - dot3(scaled, vectors)
        whole = jnp.where(index_ref[2 + block] == 1, whole, unit)
        high, low = split(whole)
        high_ref[block] = high
        low_ref[block] = low


def prepare(outer_y, index, near, after, before, far0, far1):
    blocks, quarter, m = near.shape
    n = 4 * quarter
    out = jax.ShapeDtypeStruct((blocks, m, m), jnp.bfloat16)
    vmem = pl.BlockSpec(memory_space=pltpu.VMEM)
    return pl.pallas_call(
        functools.partial(prepare_body, outer_y),
        out_shape=(out, out),
        in_specs=[pl.BlockSpec(memory_space=pltpu.SMEM)] + [vmem] * 5,
        out_specs=(vmem, vmem),
        scratch_shapes=[
            pltpu.VMEM((blocks, n, m), jnp.float32),
            pltpu.VMEM((blocks, n, n), jnp.float32),
            pltpu.VMEM((2 * blocks, n // 2, n // 2), jnp.float32),
        ],
        compiler_params=pltpu.CompilerParams(vmem_limit_bytes=14 * 1024 * 1024),
        cost_estimate=pl.CostEstimate(flops=2_000_000_000, bytes_accessed=1_000_000, transcendentals=0),
        interpret=INTERPRET,
        name="prepare",
    )(index, near, after, before, far0, far1)


PAIRS = ((0, 0), (0, 1), (0, 2), (1, 1), (1, 2), (2, 2))


def operate_body(ends_ref, data_ref, own_ref, ah, al, bh, bl, step_ref, rest_ref, add_ref):
    n = ah.shape[1] // 2
    first = ends_ref[0] == 1
    last = ends_ref[1] == 1
    width = data_ref.shape[1]
    held = {(0, 0): (ah, al, 0), (0, 1): (bh, bl, 0), (1, 0): (ah, al, 1), (1, 1): (ah, al, 2), (2, 0): (bh, bl, 1), (2, 1): (ah, al, 3)}

    def part(sweep, block, side=None):
        high, low, at = held[sweep, block]
        if side is None:
            return high[at], low[at]
        rows = pl.ds(side * n, n)
        return high[at, rows, :], low[at, rows, :]

    for sweep in range(3):
        a_top = part(sweep, 0, 0)
        b_top = part(sweep, 1, 0)
        b_low = part(sweep, 1, 1)
        fresh = a_top[0].astype(jnp.float32) + a_top[1].astype(jnp.float32)
        if sweep == 0:
            own = own_ref[...].T
            arriving = jnp.where(first, own[:, :n], 0.0)
            mid = dot3(split(jnp.concatenate([arriving, own[:, n:]], axis=1)), part(0, 0))
            mid = jnp.concatenate([fresh, mid], axis=0)
            v = data_ref[...].T
            done = dot3(split(mid[:, n:]), b_top)
            done = jnp.concatenate([done[:n], done[n:] + dot3(split(v), b_low)], axis=0)
            v = jnp.concatenate([jnp.zeros((n, n), jnp.float32), v], axis=0)
            done = jnp.where(last, jnp.concatenate([mid[:, n:], v], axis=1), done)
        else:
            mid = dot3(split(u), part(sweep, 0, 1))
            mid = jnp.concatenate([mid[:-width], fresh, mid[-width:]], axis=0)
            done = dot3(split(mid[:, n:]), b_top)
            more = dot3(split(v), b_low)
            early = sweep * n
            done = jnp.concatenate(
                [done[:early] + more[:early], done[early : early + n], done[early + n :] + more[early:]], axis=0
            )
        known = (sweep + 1) * n
        u, v = mid[:, :n], done[:, :n]
        out = done[:, n:]
        for k in range(sweep + 1):
            step_ref[PAIRS.index((k, sweep))] = out[k * n : (k + 1) * n]
        add_ref[:, sweep * n : (sweep + 1) * n] = out[known:]
    rest_ref[:, 0:n] = u[: 3 * n]
    rest_ref[:, n : 2 * n] = v[: 3 * n]
    add_ref[:, 3 * n : 4 * n] = u[3 * n :]
    add_ref[:, 4 * n : 5 * n] = v[3 * n :]

    @pl.when(last)
    def _():
        high, low = bh[0], bl[0]
        for k in range(4):
            if k < 3:
                upper = step_ref[PAIRS.index((k, 2))]
                lower = step_ref[PAIRS.index((k, 1))] if k < 2 else jnp.zeros((n, n), jnp.float32)
            else:
                upper = add_ref[:, 2 * n : 3 * n]
                lower = add_ref[:, n : 2 * n]
            result = dot3(split(jnp.concatenate([upper, lower], axis=1)), (high, low))
            if k < 3:
                rest_ref[k * n : (k + 1) * n, 2 * n :] = result
            else:
                add_ref[:, 5 * n :] = result

    @pl.when(jnp.logical_not(last))
    def _():
        rest_ref[:, 2 * n :] = jnp.zeros((3 * n, 2 * n), jnp.float32)
        add_ref[:, 5 * n :] = jnp.zeros((width, 2 * n), jnp.float32)


def operate(ends, data, own, parts):
    m, width = own.shape
    n = m // 2
    vmem = pl.BlockSpec(memory_space=pltpu.VMEM)
    return pl.pallas_call(
        operate_body,
        out_shape=(
            jax.ShapeDtypeStruct((6, n, n), jnp.float32),
            jax.ShapeDtypeStruct((3 * n, 4 * n), jnp.float32),
            jax.ShapeDtypeStruct((width, 7 * n), jnp.float32),
        ),
        in_specs=[pl.BlockSpec(memory_space=pltpu.SMEM)] + [vmem] * 6,
        out_specs=(vmem,) * 3,
        compiler_params=pltpu.CompilerParams(vmem_limit_bytes=20 * 1024 * 1024),
        interpret=INTERPRET,
        name="operate",
    )(ends, data, own, *parts)


def merge_add_body(odd_ref, mine_ref, other_ref, keep_ref, got_ref, add_ref):
    n = mine_ref.shape[1]
    odd = odd_ref[0] == 1
    wide = slice(0, 3 * n)
    keep = keep_ref[:, wide]
    got = got_ref[:, wide]
    odd_parts = [split(jnp.where(odd, mine_ref[k], other_ref[k])) for k in range(6)]
    odd_add = jnp.where(odd, keep, got)
    add_parts = split(jnp.where(odd, got, keep))
    for s in range(3):
        total = odd_add[:, s * n : (s + 1) * n]
        for j in range(s + 1):
            columns = slice(j * n, (j + 1) * n)
            total = total + dot3((add_parts[0][:, columns], add_parts[1][:, columns]), odd_parts[PAIRS.index((j, s))])
        add_ref[:, s * n : (s + 1) * n] = total


def merge_add(odd, mine, other, keep, got):
    n = mine.shape[1]
    vmem = pl.BlockSpec(memory_space=pltpu.VMEM)
    return pl.pallas_call(
        merge_add_body,
        out_shape=jax.ShapeDtypeStruct((keep.shape[0], 3 * n), jnp.float32),
        in_specs=[pl.BlockSpec(memory_space=pltpu.SMEM)] + [vmem] * 4,
        out_specs=vmem,
        compiler_params=pltpu.CompilerParams(vmem_limit_bytes=16 * 1024 * 1024),
        interpret=INTERPRET,
        name="merge_add",
    )(odd, mine, other, keep, got)


def merge_map_body(odd_ref, mine_ref, other_ref, high_ref, low_ref):
    odd = odd_ref[0] == 1
    even_parts = [split(jnp.where(odd, other_ref[k], mine_ref[k])) for k in range(6)]
    odd_parts = [split(jnp.where(odd, mine_ref[k], other_ref[k])) for k in range(6)]
    for s in range(3):
        for k in range(s + 1):
            total = None
            for j in range(k, s + 1):
                term = dot3(even_parts[PAIRS.index((k, j))], odd_parts[PAIRS.index((j, s))])
                total = term if total is None else total + term
            high_ref[PAIRS.index((k, s))], low_ref[PAIRS.index((k, s))] = split(total)


def merge_map(odd, mine, other):
    vmem = pl.BlockSpec(memory_space=pltpu.VMEM)
    packed = jax.ShapeDtypeStruct(mine.shape, jnp.bfloat16)
    return pl.pallas_call(
        merge_map_body,
        out_shape=(packed, packed),
        in_specs=[pl.BlockSpec(memory_space=pltpu.SMEM)] + [vmem] * 2,
        out_specs=(vmem,) * 2,
        compiler_params=pltpu.CompilerParams(vmem_limit_bytes=16 * 1024 * 1024),
        interpret=INTERPRET,
        name="merge_map",
    )(odd, mine, other)


def hop_body(state_ref, high_ref, low_ref, add_ref, out_ref):
    n = high_ref.shape[1]
    high, low = split(state_ref[...])
    count = high.shape[0]
    both = jnp.concatenate([high, low], axis=0)
    for s in range(3):
        total = add_ref[:, s * n : (s + 1) * n]
        for k in range(s + 1):
            at = PAIRS.index((k, s))
            columns = slice(k * n, (k + 1) * n)
            main = lax.dot_general(both[:, columns], high_ref[at], NN, preferred_element_type=jnp.float32)
            side = lax.dot_general(high[:, columns], low_ref[at], NN, preferred_element_type=jnp.float32)
            total = total + (main[:count] + (main[count:] + side))
        out_ref[:, s * n : (s + 1) * n] = total


def hop_on(state, high, low, add):
    vmem = pl.BlockSpec(memory_space=pltpu.VMEM)
    return pl.pallas_call(
        hop_body,
        out_shape=jax.ShapeDtypeStruct(state.shape, jnp.float32),
        in_specs=[vmem] * 4,
        out_specs=vmem,
        compiler_params=pltpu.CompilerParams(vmem_limit_bytes=8 * 1024 * 1024),
        interpret=INTERPRET,
        name="hop",
    )(state, high, low, add)


def ending_body(odd_ref, mine_ref, other_ref, rest_ref, other_rest_ref, keep_ref, got_ref, keep_late_ref, got_late_ref, high_ref, low_ref, add_ref):
    n = mine_ref.shape[1]
    odd = odd_ref[0] == 1
    for k in range(3):
        rows = slice(k * n, (k + 1) * n)
        even_rest = jnp.where(odd, other_rest_ref[rows, : 2 * n], rest_ref[rows, : 2 * n])
        high_ref[rows, : 2 * n], low_ref[rows, : 2 * n] = split(even_rest)
    odd_parts = []
    for k in range(3):
        rows = slice(k * n, (k + 1) * n)
        odd_parts.append(split(jnp.where(odd, rest_ref[rows, :], other_rest_ref[rows, :])))
    for k in range(3):
        total = None
        for j in range(k, 3):
            at = PAIRS.index((k, j))
            term = dot3(split(jnp.where(odd, other_ref[at], mine_ref[at])), odd_parts[j])
            total = term if total is None else total + term
        rows = slice(k * n, (k + 1) * n)
        high_ref[rows, 2 * n :], low_ref[rows, 2 * n :] = split(total)
    even_add = jnp.where(odd, got_ref[...], keep_ref[...])
    even_late = jnp.where(odd, got_late_ref[...], keep_late_ref[...])
    total = jnp.where(odd, keep_late_ref[...], got_late_ref[...])
    for j in range(3):
        total = total + dot3(split(even_add[:, j * n : (j + 1) * n]), odd_parts[j])
    add_ref[:, : 2 * n] = even_late[:, : 2 * n]
    add_ref[:, 2 * n :] = total


def ending(odd, mine, other, rest, other_rest, *adds):
    n = mine.shape[1]
    vmem = pl.BlockSpec(memory_space=pltpu.VMEM)
    wide = jax.ShapeDtypeStruct((3 * n, 6 * n), jnp.bfloat16)
    return pl.pallas_call(
        ending_body,
        out_shape=(wide, wide, jax.ShapeDtypeStruct((adds[0].shape[0], 6 * n), jnp.float32)),
        in_specs=[pl.BlockSpec(memory_space=pltpu.SMEM)] + [vmem] * 8,
        out_specs=(vmem,) * 3,
        compiler_params=pltpu.CompilerParams(vmem_limit_bytes=16 * 1024 * 1024),
        interpret=INTERPRET,
        name="ending",
    )(odd, mine, other, rest, other_rest, *adds)


def finish_body(*refs):
    *state_refs, high_ref, low_ref, add_ref, out_ref, sum_ref = refs
    hops = len(state_refs) // SUBS
    width = out_ref.shape[1]
    rows = []
    for k in range(SUBS):
        total = state_refs[k * hops][...]
        for ref in state_refs[k * hops + 1 : (k + 1) * hops]:
            total = total + ref[...]
        rows.append(total)
    state = jnp.concatenate(rows, axis=0)
    sum_ref[...] = state
    out_ref[...] = dot3(split(state), (high_ref[:, :width], low_ref[:, :width])) + add_ref[:, :width]


def finish(arrived, high, low, add):
    vmem = pl.BlockSpec(memory_space=pltpu.VMEM)
    states = [value for values in arrived for value in values]
    return pl.pallas_call(
        finish_body,
        out_shape=(
            jax.ShapeDtypeStruct((add.shape[0], add.shape[1] // 3), jnp.float32),
            jax.ShapeDtypeStruct((add.shape[0], high.shape[0]), jnp.float32),
        ),
        in_specs=[vmem] * (len(states) + 3),
        out_specs=(vmem, vmem),
        compiler_params=pltpu.CompilerParams(vmem_limit_bytes=16 * 1024 * 1024),
        interpret=INTERPRET,
        name="finish",
    )(*states, high, low, add)


def finish_own_body(state_ref, high_ref, low_ref, add_ref, even_ref, odd_ref):
    width = even_ref.shape[1]
    state = split(state_ref[...])
    for k, ref in ((1, even_ref), (2, odd_ref)):
        at = slice(k * width, (k + 1) * width)
        ref[...] = dot3(state, (high_ref[:, at], low_ref[:, at])) + add_ref[:, at]


def finish_own(state, high, low, add):
    vmem = pl.BlockSpec(memory_space=pltpu.VMEM)
    out = jax.ShapeDtypeStruct((add.shape[0], add.shape[1] // 3), jnp.float32)
    return pl.pallas_call(
        finish_own_body,
        out_shape=(out, out),
        in_specs=[vmem] * 4,
        out_specs=(vmem, vmem),
        compiler_params=pltpu.CompilerParams(vmem_limit_bytes=16 * 1024 * 1024),
        interpret=INTERPRET,
        name="finish_own",
    )(state, high, low, add)


def close_body(places_ref, got_ref, hand0_ref, hand1_ref, even_ref, odd_ref, out_ref):
    odd, last, flipped, flips_next = [places_ref[k] == 1 for k in range(4)]
    got = got_ref[...]
    for_even = even_ref[...]
    for_odd = odd_ref[...]
    near = jnp.where(flips_next, hand1_ref[...], hand0_ref[...])
    far = jnp.where(flips_next, hand0_ref[...], hand1_ref[...])
    upper = jnp.where(odd, jnp.where(last, for_odd, near), jnp.where(flipped, got, for_even))
    lower = jnp.where(odd, jnp.where(last, got, far), jnp.where(flipped, for_even, got))
    out_ref[...] = jnp.concatenate([upper, lower], axis=0).T


def close(places, got, hand0, hand1, for_even, for_odd):
    half, m = got.shape
    vmem = pl.BlockSpec(memory_space=pltpu.VMEM)
    return pl.pallas_call(
        close_body,
        out_shape=jax.ShapeDtypeStruct((m, 2 * half), jnp.float32),
        in_specs=[pl.BlockSpec(memory_space=pltpu.SMEM)] + [vmem] * 5,
        out_specs=vmem,
        compiler_params=pltpu.CompilerParams(vmem_limit_bytes=8 * 1024 * 1024),
        interpret=INTERPRET,
        name="close",
    )(places, got, hand0, hand1, for_even, for_odd)


def ring(value, axis, step):
    count = lax.axis_size(axis)
    return lax.ppermute(value, axis, [(k, (k + step) % count) for k in range(count)])


def shifted(value, step):
    count = lax.axis_size(ROW)
    return lax.ppermute(value, ROW, [(k, k + step) for k in range(max(0, -step), min(count, count - step))])


def after_these(value, others):
    return lax.optimization_barrier((value, *others))[0]


def shards(eigenvectors, householder):
    local = jnp.swapaxes(householder, 2, 3)
    position = lax.axis_index(ROW)
    count = lax.axis_size(ROW)
    chips = lax.axis_size(CHIP)
    is_first = position == 0
    is_last = position == count - 1
    is_odd = lax.axis_index("core") == 1
    middle = chips // 2
    flipped = lax.axis_index(CHIP) >= middle
    flips_next = lax.axis_index(CHIP) + 1 >= middle
    takes_second = is_odd != flipped
    on_last = lax.axis_index(CHIP) == chips - 1
    at = [lax.axis_index("y"), lax.axis_index("zh")]
    one = jnp.int32(1)
    held = jnp.where(is_first, 0, 1)
    index_a = jnp.stack([*at, one, held, one, held]).astype(jnp.int32)
    index_b = jnp.stack([*at, one, held]).astype(jnp.int32)
    ends = jnp.stack([is_first, is_last]).astype(jnp.int32)
    odd = is_odd.astype(jnp.int32).reshape(1)
    places = jnp.stack([is_odd, on_last, flipped, flips_next]).astype(jnp.int32)
    local, is_last, is_odd, takes_second, places, index_a, index_b, ends, odd = lax.optimization_barrier(
        (local, is_last, is_odd, takes_second, places, index_a, index_b, ends, odd)
    )
    n = eigenvectors.shape[0] // 2
    stay = jnp.stack([local[0, 1], local[1, 0], local[1, 1], local[2, 0]])
    half = 2 * stay.shape[1]
    before = ring(stay, "zh", 1)
    after = ring(stay, "zh", -1)
    from_next = shifted(local[0, 0], -1)
    from_prior = shifted(local[2, 1], 1)
    far = ring(before, "zh", 1)
    near_a = jnp.concatenate([stay, after, far, before], axis=1)
    moved = jnp.stack([jnp.where(is_last, local[2, 1], from_next), from_prior])
    before = ring(moved, "y", 1)
    after = ring(moved, "y", -1)
    far = ring(moved, "y", 2)
    near_b = jnp.concatenate([moved, after, far, before], axis=1)
    before_a = ring(near_a, "y", 1)
    after_a = ring(near_a, "y", -1)
    give_a0 = before_a[:, :half]
    give_a1 = after_a[:, half:]
    give_a = give_a0, give_a1
    far0_a = ring(give_a[0], "y", 1)
    far1_a = ring(give_a[1], "y", -1)
    before_b = ring(near_b, "zh", 1)
    after_b = ring(near_b, "zh", -1)
    give_b0 = before_b[:, :half]
    give_b1 = after_b[:, half:]
    give_b = after_these(give_b0, give_a), after_these(give_b1, give_a)
    far0_b = ring(give_b[0], "zh", 1)
    far1_b = ring(give_b[1], "zh", -1)
    data = shifted(after_these(eigenvectors[:n], (near_b,)), -1)
    far0_a = after_these(far0_a, give_b)
    parts_a = prepare(True, index_a, near_a, after_a, before_a, far0_a, far1_a)
    parts_b = prepare(False, index_b, after_these(near_b, parts_a), after_b, before_b, far0_b, far1_b)
    step, rest, add = operate(ends, data, eigenvectors, (*parts_a, *parts_b))

    swap = [(0, 1), (1, 0)]
    half = add.shape[0] // 2
    halves = add.reshape(2, half, 7 * n)
    mine, theirs = jnp.where(takes_second, halves[1], halves[0]), jnp.where(takes_second, halves[0], halves[1])
    keep, keep_late = mine[:, : 3 * n], mine[:, 3 * n :]
    give, give_late = theirs[:, : 3 * n], theirs[:, 3 * n :]
    other = lax.ppermute(step, "core", swap)
    got = lax.ppermute(give, "core", swap)
    rest, give_late, other, got = lax.optimization_barrier((rest, give_late, other, got))
    chip_add = merge_add(odd, step, other, keep, got)
    other_rest = lax.ppermute(rest, "core", swap)
    got_late = lax.ppermute(give_late, "core", swap)
    high, low = merge_map(odd, step, other)

    sub = half // SUBS
    adds = [chip_add[k * sub : (k + 1) * sub] for k in range(SUBS)]

    def onward(value, hop):
        turn = 1 if hop == middle else 0
        return lax.ppermute(value, ROW, [(2 * hop - 2 + side, 2 * hop + (side ^ turn)) for side in range(2)])

    arrived = []
    for k in range(SUBS):
        arrived.append([onward(adds[k], 1)])
    for hop in range(2, chips):
        for k in range(SUBS):
            sent = hop_on(arrived[k][-1], high, low, adds[k])
            arrived[k].append(onward(sent, hop))
        if hop == 4:
            ended = ending(odd, step, other, after_these(rest, [sent]), other_rest, keep, got, keep_late, got_late)
        if hop == 5:
            for values in arrived:
                values[-1] = after_these(values[-1], ended)
    for_prior, state = finish(arrived, *ended)
    handed = []
    for side in range(2):
        pairs = [(2 * (k + 1) + side, 2 * k + 1) for k in range(chips - 1)]
        handed.append(lax.ppermute(for_prior, ROW, pairs))
    for_even, for_odd = finish_own(state, *ended)
    got = lax.ppermute(jnp.where(is_odd, for_even, for_odd), "core", swap)
    return close(places, got, *handed, for_even, for_odd)


def solution(mesh):
    split_mesh = Mesh(mesh.devices.reshape(2, 4, 2, 4, 4), (*ROW, *COL))
    return jax.shard_map(
        shards,
        mesh=split_mesh,
        in_specs=(P(ROW, COL), P(None, ROW, None, COL)),
        out_specs=P(ROW, COL),
        check_vma=False,
    )
```
